32 devices in a mesh: tp: 4 (over z), side: 2 (over y), rep: 4 (over x, core).
Axes of the slice: x: 2, y: 2, z: 4, core: 2. Of those that a mesh axis runs over, the one named last changes fastest.
Arguments:
- w_up: float32 [2, 1, 2048, 8192], P('side', None, ('rep', 'tp'))
- w_down: float32 [2, 1, 8192, 2048], P('side', None, None, ('rep', 'tp'))
- g_up: float32 [2, 1, 2048, 8192], P('side', None, ('rep', 'tp'))
- g_down: float32 [2, 1, 8192, 2048], P('side', None, None, ('rep', 'tp'))
- learn_rate: float32 [2], P('side')
- prompts: bfloat16 [2, 4, 8192, 2048], P('side', 'rep')
Outputs:
- output 1: float32 [2, 1, 2048, 8192], P('side', None, ('rep', 'tp'))
- output 2: float32 [2, 1, 8192, 2048], P('side', None, None, ('rep', 'tp'))
- output 3: bfloat16 [2, 4, 8192, 2048], P('side', 'rep')
All inputs are finite; a program needn't handle non-finite values.
Results may differ from the reference program's by a relative error of at most 0.001.
Values are sent between devices in bfloat16 or wider.
A program may use at most 1 GiB of HBM per device.

```python
import jax
import jax.numpy as jnp
from jax import lax

NUM_LAYERS = 1
MODEL_DIM = 2048
HIDDEN_DIM = 8192
NUM_REPS = 4
NUM_TOKENS = 8192


def setup_inputs(seed: int = 0) -> dict:
    keys = jax.random.split(jax.random.key(seed), 6)
    up_shape = (NUM_LAYERS, MODEL_DIM, HIDDEN_DIM)
    down_shape = (NUM_LAYERS, HIDDEN_DIM, MODEL_DIM)
    up_scale = MODEL_DIM ** -0.5
    down_scale = (2.0 / (HIDDEN_DIM * NUM_LAYERS)) ** 0.5
    w_up = jax.random.normal(keys[0], up_shape, jnp.float32) * up_scale
    w_down = jax.random.normal(keys[1], down_shape, jnp.float32) * down_scale
    g_up = jax.random.normal(keys[2], up_shape, jnp.float32) * up_scale
    g_down = jax.random.normal(keys[3], down_shape, jnp.float32) * down_scale
    rate = jax.random.uniform(keys[4], (1,), jnp.float32, 0.04, 0.2)
    prompts = jax.random.normal(keys[5], (NUM_REPS, NUM_TOKENS, MODEL_DIM), jnp.float32)
    zero_up = jnp.zeros(up_shape, jnp.float32)
    zero_down = jnp.zeros(down_shape, jnp.float32)
    return {
        "w_up": jnp.stack([w_up, zero_up]),
        "w_down": jnp.stack([w_down, zero_down]),
        "g_up": jnp.stack([g_up, zero_up]),
        "g_down": jnp.stack([g_down, zero_down]),
        "learn_rate": jnp.concatenate([rate, jnp.zeros((1,), jnp.float32)]),
        "prompts": jnp.stack([jnp.zeros_like(prompts), prompts]).astype(jnp.bfloat16),
    }


def reference(w_up, w_down, g_up, g_down, learn_rate, prompts):
    rate = learn_rate[0]
    new_up = w_up[0] - rate * g_up[0]
    new_down = w_down[0] - rate * g_down[0]
    cast_up = new_up.astype(jnp.bfloat16)
    cast_down = new_down.astype(jnp.bfloat16)

    def layer_step(hidden, weights):
        up_mat, down_mat = weights
        pre_act = jnp.dot(hidden, up_mat, preferred_element_type=jnp.float32)
        act_up = jax.nn.gelu(pre_act, approximate=True).astype(jnp.bfloat16)
        part_sum = jnp.dot(act_up, down_mat, preferred_element_type=jnp.float32)
        return (hidden.astype(jnp.float32) + part_sum).astype(jnp.bfloat16), None

    def replica_forward(rows):
        return lax.scan(layer_step, rows, (cast_up, cast_down))[0]

    gen_out = lax.map(replica_forward, prompts[1])
    up_out = jnp.stack([new_up, jnp.zeros_like(new_up)])
    down_out = jnp.stack([new_down, jnp.zeros_like(new_down)])
    tok_out = jnp.stack([jnp.zeros_like(gen_out), gen_out])
    return (up_out, down_out, tok_out)
```

```python
import functools
import math

import jax
import jax.numpy as jnp
from jax import lax
from jax.experimental import pallas as pl
from jax.experimental.pallas import tpu as pltpu
from jax.sharding import PartitionSpec as P

BF, F32 = jnp.bfloat16, jnp.float32
MESH = pl.DeviceIdType.MESH
D, F, TOK = 2048, 8192, 8192
FC = 256
NCH = F // FC
FS = 512
NST = F // FS
M = 1024
R1 = 3 * M
R2 = TOK - 2 * R1
PC = 256
NPC = R1 // PC
AHEAD = 3
LAGX, LAGD = 1, 3


def gelu(a):
    k = math.sqrt(2.0 / math.pi)
    half = 0.5 * a
    return half + half * jnp.tanh(a * (k + (k * 0.044715) * (a * a)))


def kernel(
    wu_in, wd_in, rows_in, out, w_all, relay, h, acc, wu, wd,
    y_sem, x_sem, b_sem, d_sem, s1, s2, s3, sb, ld_sem, h_sem, o_sem, e_recv, e_send, r_recv,
):
    t, side, r = lax.axis_index("tp"), lax.axis_index("side"), lax.axis_index("rep")
    x, c = r // 2, r % 2

    def send(src, dst, send_sem, recv_sem, device):
        pltpu.make_async_remote_copy(
            src, dst, send_sem, recv_sem, device_id=device, device_id_type=MESH
        ).start()

    def wait(ref, sem):
        pltpu.make_async_copy(ref, ref, sem).wait()

    def kind(ch):
        m = (ch * 7) % 16
        return m < 7, jnp.logical_and(m >= 7, m < 11), m >= 11

    def valid(ch):
        return jnp.logical_and(ch >= 0, ch < NCH)

    def up(ch, col, j):
        return w_all.at[ch, c, col, 0, pl.ds(j * 128, 128), :]

    def down(ch, col, j):
        return w_all.at[ch, c, col, 1, pl.ds((j // 2) * 256, 256), pl.ds((j % 2) * 128, 128)]

    def up2(ch, j):
        return w_all.at[ch, c, :, 0, pl.ds(j * 128, 128), :]

    def down2(ch, j):
        return w_all.at[ch, c, :, 1, pl.ds((j // 2) * 256, 256), pl.ds((j % 2) * 128, 128)]

    def one_band(ch):
        return w_all.at[ch, 0, 0, 0, pl.ds(0, 256), :]

    def two_bands(ch):
        return w_all.at[ch, 0, 0, 0]

    def unit(ch):
        return w_all.at[ch, 0, 0]

    def pair(ch):
        return w_all.at[ch, 0]

    @pl.when(side == 0)
    def _():
        def along(ch, j, right, su, sd, sem):
            dev = (t + 1, 0, r) if right else (t - 1, 0, r)
            send(su, up(ch, x, j), sem, b_sem.at[ch, j], dev)
            send(sd, down(ch, x, j), sem, b_sem.at[ch, j], dev)

        def across(ch, col, j, su, sd):
            send(su, up(ch, col, j), s1.at[ch], y_sem.at[ch], (t, 1, r))
            send(sd, down(ch, col, j), s1.at[ch], y_sem.at[ch], (t, 1, r))

        def slot(i, _):
            e = i - AHEAD
            chz = e + AHEAD
            is_a, is_b, is_g = kind(chz)
            f0 = pl.multiple_of(jnp.minimum(chz, NCH - 1) * FC, FC)
            su, sd = wu_in.at[:, pl.ds(f0, FC)], wd_in.at[pl.ds(f0, FC), :]

            @pl.when(jnp.logical_and(valid(chz), jnp.logical_not(is_a)))
            def _():
                across(chz, x, t, su, sd)

                @pl.when(is_g)
                def _():
                    send(su, up(chz, x, t), s2.at[chz], x_sem.at[chz], (t, 0, r ^ 2))
                    send(sd, down(chz, x, t), s2.at[chz], x_sem.at[chz], (t, 0, r ^ 2))

            cha = e
            is_a, _, _ = kind(cha)
            f1 = pl.multiple_of(jnp.maximum(jnp.minimum(cha, NCH - 1), 0) * FC, FC)
            su1, sd1 = wu_in.at[:, pl.ds(f1, FC)], wd_in.at[pl.ds(f1, FC), :]

            @pl.when(jnp.logical_and(valid(cha), is_a))
            def _():
                across(cha, x, t, su1, sd1)

                @pl.when(t < 3)
                def _():
                    along(cha, t, True, su1, sd1, sb.at[cha, t])

                @pl.when(t > 0)
                def _():
                    along(cha, t, False, su1, sd1, s3.at[cha])

            for k in (1, 2, 3):
                ch = e - k
                is_a, _, _ = kind(ch)
                go = jnp.logical_and(valid(ch), is_a)

                @pl.when(jnp.logical_and(go, t >= k))
                def _():
                    j = t - k
                    wait(one_band(ch), b_sem.at[ch, j])
                    across(ch, x, j, up(ch, x, j), down(ch, x, j))

                    @pl.when(t < 3)
                    def _():
                        along(ch, j, True, up(ch, x, j), down(ch, x, j), sb.at[ch, j])

                @pl.when(jnp.logical_and(go, t + k <= 3))
                def _():
                    j = t + k
                    wait(one_band(ch), b_sem.at[ch, j])
                    across(ch, x, j, up(ch, x, j), down(ch, x, j))

                    @pl.when(t > 0)
                    def _():
                        along(ch, j, False, up(ch, x, j), down(ch, x, j), sb.at[ch, j])

            chg = e + AHEAD - 1
            _, _, is_g = kind(chg)

            @pl.when(jnp.logical_and(valid(chg), is_g))
            def _():
                wait(one_band(chg), x_sem.at[chg])
                across(chg, 1 - x, t, up(chg, 1 - x, t), down(chg, 1 - x, t))

            return 0

        lax.fori_loop(0, NCH + AHEAD + 4, slot, 0)

        h[pl.ds(0, M), :] = jnp.zeros((M, D), BF)
        for i in range(TOK // M):
            pltpu.make_async_copy(h.at[pl.ds(0, M)], out.at[pl.ds(i * M, M)], o_sem).start()

        @pl.when(jnp.logical_or(t == 1, t == 2))
        def _():
            base = jnp.where(t == 1, R1, 0)
            end = jnp.where(t == 1, 0, 3)
            odd = t - 1

            def piece(i, _):
                wait(relay.at[i], r_recv.at[i])
                row = pl.multiple_of(base + (2 * i + odd) * PC, PC)
                send(relay.at[i], out.at[pl.ds(row, PC)], e_send.at[2], e_recv.at[odd], (end, 1, r))
                return 0

            lax.fori_loop(0, NPC // 2, piece, 0)
            wait(relay, e_send.at[2])

        def drain(ch, _):
            is_a, is_b, is_g = kind(ch)

            @pl.when(is_a)
            def _():
                wait(unit(ch), s1.at[ch])

                @pl.when(t > 0)
                def _():
                    wait(one_band(ch), s3.at[ch])

                for j in range(4):
                    hops = jnp.logical_or(
                        jnp.logical_and(j <= t, t < 3), jnp.logical_and(j > t, t > 0)
                    )

                    @pl.when(hops)
                    def _():
                        wait(one_band(ch), sb.at[ch, j])

            @pl.when(is_b)
            def _():
                wait(one_band(ch), s1.at[ch])

            @pl.when(is_g)
            def _():
                wait(two_bands(ch), s1.at[ch])
                wait(one_band(ch), s2.at[ch])

            return 0

        lax.fori_loop(0, NCH, drain, 0)
        wait(out, o_sem)

    @pl.when(side == 1)
    def _():
        sib, opp = (t, 1, r ^ 1), (t, 1, r ^ 2)
        base = jnp.where(t % 2 == 0, 0, R1)

        def over(ref, ch, dev):
            send(ref, ref, s1.at[ch], d_sem.at[ch], dev)

        def hop(ch, j, right, sem, is_b, is_g):
            dev = (t + 1, 1, r) if right else (t - 1, 1, r)

            @pl.when(is_b)
            def _():
                for ref in (up(ch, x, j), down(ch, x, j)):
                    send(ref, ref, sem, b_sem.at[ch, j], dev)

            @pl.when(is_g)
            def _():
                for ref in (up2(ch, j), down2(ch, j)):
                    send(ref, ref, sem, b_sem.at[ch, j], dev)

        def tick(e):
            is_a, _, _ = kind(e)
            own = w_all.at[e, c, x]

            @pl.when(jnp.logical_and(valid(e), is_a))
            def _():
                wait(unit(e), y_sem.at[e])
                send(own, own, s2.at[e], x_sem.at[e], opp)
                over(own, e, sib)

            ch = e + AHEAD
            is_a, is_b, is_g = kind(ch)

            @pl.when(jnp.logical_and(valid(ch), jnp.logical_not(is_a)))
            def _():
                @pl.when(is_b)
                def _():
                    wait(one_band(ch), y_sem.at[ch])

                @pl.when(is_g)
                def _():
                    wait(two_bands(ch), y_sem.at[ch])

                @pl.when(t < 3)
                def _():
                    hop(ch, t, True, sb.at[ch, t], is_b, is_g)

                @pl.when(t > 0)
                def _():
                    hop(ch, t, False, s3.at[ch], is_b, is_g)

            for k in (1, 2, 3):
                chk = e + AHEAD - k
                is_a, kb, kg = kind(chk)
                go = jnp.logical_and(valid(chk), jnp.logical_not(is_a))

                def arrive(j):
                    @pl.when(kb)
                    def _():
                        wait(one_band(chk), b_sem.at[chk, j])

                    @pl.when(kg)
                    def _():
                        wait(two_bands(chk), b_sem.at[chk, j])

                @pl.when(jnp.logical_and(go, t >= k))
                def _():
                    arrive(t - k)

                    @pl.when(t < 3)
                    def _():
                        hop(chk, t - k, True, sb.at[chk, t - k], kb, kg)

                @pl.when(jnp.logical_and(go, t + k <= 3))
                def _():
                    arrive(t + k)

                    @pl.when(t > 0)
                    def _():
                        hop(chk, t + k, False, sb.at[chk, t + k], kb, kg)

            ch3 = e + AHEAD - 3
            _, is_b, is_g = kind(ch3)

            @pl.when(jnp.logical_and(valid(ch3), is_b))
            def _():
                mine = w_all.at[ch3, c, x]
                send(mine, mine, s2.at[ch3], x_sem.at[ch3], opp)
                over(mine, ch3, sib)

            @pl.when(jnp.logical_and(valid(ch3), is_g))
            def _():
                over(w_all.at[ch3, c], ch3, sib)

            chx = e - LAGX
            _, _, is_g = kind(chx)

            @pl.when(jnp.logical_and(valid(chx), jnp.logical_not(is_g)))
            def _():
                wait(unit(chx), x_sem.at[chx])
                over(w_all.at[chx, c, 1 - x], chx, sib)

        def load(ch, slot, half, start):
            for cc in range(2):
                for xx in range(2):
                    d0 = (2 * xx + cc) * 512
                    cps = [
                        pltpu.make_async_copy(
                            w_all.at[ch, cc, xx, 0],
                            wu.at[slot, pl.ds(d0, 512), pl.ds(half * FC, FC)],
                            ld_sem.at[slot, half, 0],
                        )
                    ]
                    for q in range(2):
                        cps.append(
                            pltpu.make_async_copy(
                                w_all.at[ch, cc, xx, 1, pl.ds(q * 256, 256), :],
                                wd.at[slot, pl.ds(half * FC, FC), pl.ds(d0 + q * 256, 256)],
                                ld_sem.at[slot, half, 1],
                            )
                        )
                    for cp in cps:
                        cp.start()

        def loaded(slot, half):
            wait(wu.at[slot, :, pl.ds(half * FC, FC)], ld_sem.at[slot, half, 0])
            wait(wd.at[slot, pl.ds(half * FC, FC), :], ld_sem.at[slot, half, 1])

        def fetch(row, n, dst):
            return pltpu.make_async_copy(rows_in.at[pl.ds(row, n)], h.at[pl.ds(dst, n)], h_sem)

        def ready(ch):
            wait(pair(ch), d_sem.at[ch])

        first = fetch(pl.multiple_of(base, M), R1, 0)
        first.start()

        def zero(i, _):
            acc[pl.ds(pl.multiple_of(i * 256, 256), 256), :] = jnp.zeros((256, D), F32)
            return 0

        lax.fori_loop(0, R1 // 256, zero, 0)
        first.wait()

        e0 = LAGD + 2
        lax.fori_loop(-AHEAD, e0, lambda e, _: (tick(e), 0)[1], 0)
        for half in range(2):
            ready(half)
            load(half, 0, half, True)

        def give(i):
            @pl.when(i >= 0)
            def _():
                for q in range(M // PC):
                    p = i * (M // PC) + q
                    src = out.at[pl.ds(pl.multiple_of(base + p * PC, PC), PC)]
                    if q % 2 == 0:

                        @pl.when(t < 3)
                        def _():
                            send(src, src, e_send.at[0], e_recv.at[0], (t + 1, 1, r))

                        @pl.when(t == 1)
                        def _():
                            i2 = i * (M // PC // 2) + q // 2
                            send(src, relay.at[i2], e_send.at[2], r_recv.at[i2], (t, 0, r))
                    else:

                        @pl.when(t > 0)
                        def _():
                            send(src, src, e_send.at[1], e_recv.at[1], (t - 1, 1, r))

                        @pl.when(t == 2)
                        def _():
                            i2 = i * (M // PC // 2) + q // 2
                            send(src, relay.at[i2], e_send.at[2], r_recv.at[i2], (t, 0, r))

        def step(sp, _):
            pas, st, slot = sp // NST, sp % NST, sp % 2
            for half in range(2):
                loaded(slot, half)

            @pl.when(sp == NST)
            def _():
                wait(h.at[pl.ds(0, R2)], h_sem)

            def block(i, _):
                rs = pl.ds(pl.multiple_of(i * M, M), M)

                @pl.when(i < 2)
                def _():
                    n = 2 * (sp + 1) + i

                    @pl.when(n < NCH + 2)
                    def _():
                        tick(e0 + n - 2)

                    @pl.when(n < NCH)
                    def _():
                        ready(n)

                    @pl.when(n < 2 * NCH)
                    def _():
                        for half in range(2):

                            @pl.when(i == half)
                            def _():
                                load(n % NCH, 1 - slot, half, True)

                @pl.when(jnp.logical_and(sp == NST - 1, i > 0))
                def _():
                    wait(h.at[pl.ds(0, M)], o_sem)
                    give(i - 1)
                    j = pl.multiple_of((i - 1) * M, M)
                    fetch(2 * R1 + j, M, j).start()

                a = jnp.dot(h[rs, :], wu[slot], preferred_element_type=F32)
                u = gelu(a).astype(BF)
                for q in range(2):
                    cs = pl.ds(q * (D // 2), D // 2)
                    acc[rs, cs] += jnp.dot(u, wd[slot, :, cs], preferred_element_type=F32)

                @pl.when(st == NST - 1)
                def _():
                    def fin(q, _):
                        qs = pl.ds(pl.multiple_of(i * M + q * 128, 128), 128)
                        h[qs, :] = (h[qs, :].astype(F32) + acc[qs, :]).astype(BF)
                        acc[qs, :] = jnp.zeros((128, D), F32)
                        return 0

                    lax.fori_loop(0, M // 128, fin, 0)
                    row = pl.multiple_of(jnp.where(pas == 0, base, 2 * R1) + i * M, M)
                    pltpu.make_async_copy(h.at[rs], out.at[pl.ds(row, M)], o_sem).start()

                return 0

            lax.fori_loop(0, 3 - pas, block, 0)

            @pl.when(sp == NST - 1)
            def _():
                wait(h.at[pl.ds(0, M)], o_sem)
                give(R1 // M - 1)

            return 0

        lax.fori_loop(0, 2 * NST, step, 0)
        wait(h.at[pl.ds(0, R2)], o_sem)

        half_rows = out.at[pl.ds(0, R1 // 2)]
        wait(half_rows, e_recv.at[0])
        wait(half_rows, e_recv.at[1])

        @pl.when(t < 3)
        def _():
            wait(half_rows, e_send.at[0])

        @pl.when(t > 0)
        def _():
            wait(half_rows, e_send.at[1])

        @pl.when(jnp.logical_or(t == 1, t == 2))
        def _():
            wait(half_rows, e_send.at[2])

        def drain(ch, _):
            is_a, is_b, is_g = kind(ch)
            wait(pair(ch), s1.at[ch])

            @pl.when(jnp.logical_not(is_g))
            def _():
                wait(unit(ch), s2.at[ch])

            for size, on in ((one_band, is_b), (two_bands, is_g)):

                @pl.when(on)
                def _():
                    @pl.when(t > 0)
                    def _():
                        wait(size(ch), s3.at[ch])

                    for j in range(4):
                        hops = jnp.logical_or(
                            jnp.logical_and(j <= t, t < 3), jnp.logical_and(j > t, t > 0)
                        )

                        @pl.when(hops)
                        def _():
                            wait(size(ch), sb.at[ch, j])

            return 0

        lax.fori_loop(0, NCH, drain, 0)


def sync_and_run(wu, wd, rows):
    dma = pltpu.SemaphoreType.DMA
    any_ = pl.BlockSpec(memory_space=pl.ANY)
    out, _, _ = pl.pallas_call(
        kernel,
        out_shape=(
            jax.ShapeDtypeStruct((TOK, D), BF),
            jax.ShapeDtypeStruct((NCH, 2, 2, 2, 512, FC), BF),
            jax.ShapeDtypeStruct((NPC // 2, PC, D), BF),
        ),
        in_specs=[any_] * 3,
        out_specs=(any_,) * 3,
        scratch_shapes=[
            pltpu.VMEM((R1, D), BF),
            pltpu.VMEM((R1, D), F32),
            pltpu.VMEM((2, D, FS), BF),
            pltpu.VMEM((2, FS, D), BF),
            dma((NCH,)), dma((NCH,)), dma((NCH, 4)), dma((NCH,)),
            dma((NCH,)), dma((NCH,)), dma((NCH,)), dma((NCH, 4)),
            dma((2, 2, 2)), dma(()), dma(()), dma((2,)), dma((3,)), dma((NPC // 2,)),
        ],
        compiler_params=pltpu.CompilerParams(
            has_side_effects=True, vmem_limit_bytes=67043328
        ),
        name="sync_and_run",
    )(wu, wd, rows)
    return out


def solution(mesh):
    up_spec = P("side", None, ("rep", "tp"), None)
    down_spec = P("side", None, None, ("rep", "tp"))
    tok_spec = P("side", "rep", None, None)

    def device_step(w_up, w_down, g_up, g_down, learn_rate, prompts):
        rate = learn_rate[0]
        new_up = w_up - rate * g_up
        new_down = w_down - rate * g_down
        out = sync_and_run(new_up[0, 0].astype(BF), new_down[0, 0].astype(BF), prompts[0, 0])
        return new_up, new_down, out[None, None]

    return jax.shard_map(
        device_step,
        mesh=mesh,
        in_specs=(up_spec, down_spec, up_spec, down_spec, P("side"), tok_spec),
        out_specs=(up_spec, down_spec, tok_spec),
        check_vma=False,
    )
```

```python
import functools
import math

import jax
import jax.numpy as jnp
from jax import lax
from jax.experimental import pallas as pl
from jax.experimental.pallas import tpu as pltpu
from jax.sharding import PartitionSpec as P

BF, F32 = jnp.bfloat16, jnp.float32
MESH = pl.DeviceIdType.MESH
D, F, TOK = 2048, 8192, 8192
FC = 128
NCH = F // FC
QS = 4
NST = NCH // QS
M1 = 768
R1 = QS * M1
R2 = TOK - 2 * R1
M2 = R2 // 2
PC = 128
NPC = R1 // PC
N_A, N_B, MUL, OFF = 30, 14, 19, 2
N_G = NCH - N_A - N_B
B0 = 8


def gelu(a):
    k = math.sqrt(2.0 / math.pi)
    half = 0.5 * a
    return half + half * jnp.tanh(a * (k + (k * 0.044715) * (a * a)))


def reached(b):
    n, left = b + B0, jnp.maximum(0, NCH - 5 - b)

    def lead(most, at_first):
        return jnp.minimum(most, jnp.minimum(at_first + lax.div(3 * jnp.maximum(n, 0), 2), 2 * left))

    x = lead(1, 1)
    h3 = jnp.maximum(x, lead(3, 3))
    h2 = jnp.maximum(h3, lead(5, 4))
    h1 = jnp.maximum(h2, lead(7, 5))
    yz = jnp.maximum(h1, lead(9, 6))
    ya = jnp.maximum(x, lead(4, 2))
    return [
        jnp.where(n < 0, 0, jnp.clip(b + 5 + v, 0, NCH)) for v in (ya, yz, h1, h2, h3, x, 0)
    ]


def spans(b):
    return list(zip(reached(b - 1), reached(b)))


def each(span, body):
    lax.fori_loop(span[0], span[1], lambda ch, _: (body(ch), 0)[1], 0)


def kernel(
    rate, wu_in, gu_in, wd_in, gd_in, rows_in, out, w_all, relay, h, h2, acc, wv,
    y_sem, x_sem, b_sem, d_sem, s_over, s_opp, s_y, s_z, ld_sem, up_sem, h_sem, o_sem,
    e_recv, e_send, r_recv,
):
    t, side, r = lax.axis_index("tp"), lax.axis_index("side"), lax.axis_index("rep")
    x, c = r // 2, r % 2

    def send(src, dst, send_sem, recv_sem, device):
        pltpu.make_async_remote_copy(
            src, dst, send_sem, recv_sem, device_id=device, device_id_type=MESH
        ).start()

    def wait(ref, sem):
        pltpu.make_async_copy(ref, ref, sem).wait()

    def kind(ch):
        m = lax.rem((ch + OFF) * MUL, NCH)
        return m < N_A, jnp.logical_and(m >= N_A, m < N_A + N_B), m >= N_A + N_B

    def band(ch, col, j):
        return w_all.at[ch, c, col, :, pl.ds(j * 128, 128), :]

    def band2(ch, j):
        return w_all.at[ch, c, :, :, pl.ds(j * 128, 128), :]

    def amount(n):
        if n % 16 == 0:
            return w_all.at[pl.ds(0, n // 16)]
        if n % 8 == 0:
            return w_all.at[pl.ds(0, n // 8), 0]
        if n % 4 == 0:
            return w_all.at[pl.ds(0, n // 4), 0, 0]
        if n % 2 == 0:
            return w_all.at[pl.ds(0, n // 2), 0, 0, 0]
        return w_all.at[pl.ds(0, n), 0, 0, 0, pl.ds(0, 256), :]

    @pl.when(side == 0)
    def _():
        def parts(g):
            s = g % 2
            f0 = pl.multiple_of(g * QS * FC, QS * FC)
            cols, rows = pl.ds(f0, QS * FC), pl.ds(f0, QS * FC)
            up, dn = pl.ds(128 * s, 128), pl.ds(512 + 512 * s, 512)
            return [
                pltpu.make_async_copy(src, dst, up_sem.at[s, k])
                for k, (src, dst) in enumerate(
                    (
                        (wu_in.at[:, cols], acc.at[up, pl.ds(0, 512)]),
                        (gu_in.at[:, cols], acc.at[up, pl.ds(512, 512)]),
                        (wd_in.at[rows, :], acc.at[dn, pl.ds(0, 128)]),
                        (gd_in.at[rows, :], acc.at[dn, pl.ds(128, 128)]),
                    )
                )
            ]

        def update(g):
            s = g % 2
            for cp in parts(g):
                cp.wait()

            @pl.when(g + 1 < NST)
            def _():
                for cp in parts(g + 1):
                    cp.start()

            lr = rate[0]
            up = pl.ds(pl.multiple_of(128 * s, 128), 128)
            new_up = (acc[up, 0:512] - lr * acc[up, 512:1024]).astype(BF)
            for q in range(QS):
                wv[QS * s + q, 0, 0, 0, 0:128, :] = new_up[:, q * FC : (q + 1) * FC]
                dn = pl.ds(pl.multiple_of(512 + 512 * s + q * FC, FC), FC)
                new_dn = (acc[dn, 0:128] - lr * acc[dn, 128:256]).astype(BF)
                wv[QS * s + q, 0, 0, 1, 0:128, :] = new_dn
            cp = pltpu.make_async_copy(
                wv.at[pl.ds(QS * s, QS), 0, 0, :, pl.ds(0, 128), :],
                w_all.at[pl.ds(QS * g, QS), c, x, :, pl.ds(t * 128, 128), :],
                o_sem,
            )
            cp.start()
            cp.wait()

        def along(ch, j, right):
            if right:
                send(band(ch, x, j), band(ch, x, j), s_z.at[0, 0], b_sem.at[ch, j], (t + 1, 0, r))
            else:
                send(band(ch, x, j), band(ch, x, j), s_z.at[1, 0], b_sem.at[ch, j], (t - 1, 0, r))

        def across(ch, col, j, k):
            send(band(ch, col, j), band(ch, col, j), s_y.at[k], y_sem.at[ch], (t, 1, r))

        def own_a(ch):
            @pl.when(kind(ch)[0])
            def _():
                across(ch, x, t, 0)

                @pl.when(t < 3)
                def _():
                    along(ch, t, True)

                @pl.when(t > 0)
                def _():
                    along(ch, t, False)

        def own_z(ch):
            is_a, _, is_g = kind(ch)

            @pl.when(jnp.logical_not(is_a))
            def _():
                across(ch, x, t, 1)

            @pl.when(is_g)
            def _():
                send(band(ch, x, t), band(ch, x, t), s_opp, x_sem.at[ch], (t, 0, r ^ 2))

        def from_opp(ch):
            @pl.when(kind(ch)[2])
            def _():
                wait(amount(1), x_sem.at[ch])
                across(ch, 1 - x, t, 1)

        def hop(k):
            def body(ch):
                is_a = kind(ch)[0]

                @pl.when(jnp.logical_and(is_a, t >= k))
                def _():
                    wait(amount(1), b_sem.at[ch, t - k])
                    across(ch, x, t - k, 0)

                    @pl.when(t < 3)
                    def _():
                        along(ch, t - k, True)

                @pl.when(jnp.logical_and(is_a, t + k <= 3))
                def _():
                    wait(amount(1), b_sem.at[ch, t + k])
                    across(ch, x, t + k, 0)

                    @pl.when(t > 0)
                    def _():
                        along(ch, t + k, False)

            return body

        for cp in parts(0):
            cp.start()

        def slot(b, done):
            ya, yz = spans(b)[:2]
            todo = (jnp.maximum(ya[1], yz[1]) + QS - 1) // QS
            each((done, todo), update)
            each(ya, own_a)
            each(yz, own_z)

            @pl.when(b == -B0)
            def _():
                for k in (1, 2, 3):
                    each(ya, hop(k))

            for k in (1, 2, 3):
                lo, hi = spans(b - k)[0]
                each((lo, jnp.where(b - k > -B0, hi, lo)), hop(k))
            each(yz, from_opp)
            return todo

        lax.fori_loop(-B0, NCH + 4, slot, 0)

        @pl.when(jnp.logical_or(t == 1, t == 2))
        def _():
            base = jnp.where(t == 1, R1, 0)
            end = jnp.where(t == 1, 0, 3)
            odd = t - 1

            def piece(i, _):
                wait(relay.at[i], r_recv.at[i])
                row = pl.multiple_of(base + (2 * i + odd) * PC, PC)
                send(relay.at[i], out.at[pl.ds(row, PC)], e_send.at[2], e_recv.at[odd], (end, 1, r))
                return 0

            lax.fori_loop(0, NPC // 2, piece, 0)
            wait(relay, e_send.at[2])

        wait(amount(4 * N_A), s_y.at[0])
        wait(amount(N_B + 2 * N_G), s_y.at[1])
        wait(amount(N_G), s_opp)
        for tt in range(4):

            @pl.when(t == tt)
            def _():
                if tt < 3:
                    wait(amount((tt + 1) * N_A), s_z.at[0, 0])
                if tt > 0:
                    wait(amount((4 - tt) * N_A), s_z.at[1, 0])


    @pl.when(side == 1)
    def _():
        sib, opp = (t, 1, r ^ 1), (t, 1, r ^ 2)
        base = jnp.where(t % 2 == 0, 0, R1)

        def over(ref, ch):
            send(ref, ref, s_over, d_sem.at[ch], sib)

        def along(ch, j, right, is_b, is_g):
            k = 0 if right else 1
            dev = (t + 1, 1, r) if right else (t - 1, 1, r)

            @pl.when(is_b)
            def _():
                send(band(ch, x, j), band(ch, x, j), s_z.at[k, 0], b_sem.at[ch, j], dev)

            @pl.when(is_g)
            def _():
                send(band2(ch, j), band2(ch, j), s_z.at[k, 1], b_sem.at[ch, j], dev)

        def arrive(sem, is_b, is_g):
            @pl.when(is_b)
            def _():
                wait(amount(1), sem)

            @pl.when(is_g)
            def _():
                wait(amount(2), sem)

        def across(ch):
            own = w_all.at[ch, c, x]
            send(own, own, s_opp, x_sem.at[ch], opp)
            over(own, ch)

        def ya(ch):
            @pl.when(kind(ch)[0])
            def _():
                wait(amount(4), y_sem.at[ch])
                across(ch)

        def yz(ch):
            is_a, is_b, is_g = kind(ch)

            @pl.when(jnp.logical_not(is_a))
            def _():
                arrive(y_sem.at[ch], is_b, is_g)

                @pl.when(t < 3)
                def _():
                    along(ch, t, True, is_b, is_g)

                @pl.when(t > 0)
                def _():
                    along(ch, t, False, is_b, is_g)

        def hop(k):
            def body(ch):
                is_a, is_b, is_g = kind(ch)

                @pl.when(jnp.logical_and(jnp.logical_not(is_a), t >= k))
                def _():
                    arrive(b_sem.at[ch, t - k], is_b, is_g)

                    @pl.when(t < 3)
                    def _():
                        along(ch, t - k, True, is_b, is_g)

                @pl.when(jnp.logical_and(jnp.logical_not(is_a), t + k <= 3))
                def _():
                    arrive(b_sem.at[ch, t + k], is_b, is_g)

                    @pl.when(t > 0)
                    def _():
                        along(ch, t + k, False, is_b, is_g)

                if k == 3:

                    @pl.when(is_b)
                    def _():
                        across(ch)

                    @pl.when(is_g)
                    def _():
                        over(w_all.at[ch, c], ch)

            return body

        def from_opp(ch):
            @pl.when(jnp.logical_not(kind(ch)[2]))
            def _():
                wait(amount(4), x_sem.at[ch])
                over(w_all.at[ch, c, 1 - x], ch)

        def load(ch, ring):
            pltpu.make_async_copy(w_all.at[ch], wv.at[ring], ld_sem.at[ring]).start()

        def ready(ch):
            wait(amount(8), d_sem.at[ch])
            load(ch, ch % (2 * QS))

        def tick(b):
            stages = (ya, yz, hop(1), hop(2), hop(3), from_opp, ready)
            for span, stage in zip(spans(b), stages):
                each(span, stage)

        def loaded(slot):
            for q in range(QS):
                wait(wv.at[QS * slot + q], ld_sem.at[QS * slot + q])

        def store(ref, row, n, to):
            return pltpu.make_async_copy(ref.at[pl.ds(row, n)], out.at[pl.ds(to, n)], o_sem)

        first = pltpu.make_async_copy(
            rows_in.at[pl.ds(pl.multiple_of(base, 1024), R1)], h, h_sem.at[0]
        )
        second = pltpu.make_async_copy(rows_in.at[pl.ds(2 * R1, R2)], h2, h_sem.at[1])
        first.start()
        second.start()

        def zero(i, _):
            acc[pl.ds(pl.multiple_of(i * 128, 128), 128), :] = jnp.zeros((128, D), F32)
            return 0

        lax.fori_loop(0, R1 // 128, zero, 0)
        first.wait()
        lax.fori_loop(-B0, 0, lambda b, _: (tick(b), 0)[1], 0)

        def give(i):
            for q in range(M1 // PC):
                p = i * (M1 // PC) + q
                src = out.at[pl.ds(pl.multiple_of(base + p * PC, PC), PC)]
                i2 = i * (M1 // PC // 2) + q // 2
                if q % 2 == 0:

                    @pl.when(t < 3)
                    def _():
                        send(src, src, e_send.at[0], e_recv.at[0], (t + 1, 1, r))

                    @pl.when(t == 1)
                    def _():
                        send(src, relay.at[i2], e_send.at[2], r_recv.at[i2], (t, 0, r))
                else:

                    @pl.when(t > 0)
                    def _():
                        send(src, src, e_send.at[1], e_recv.at[1], (t - 1, 1, r))

                    @pl.when(t == 2)
                    def _():
                        send(src, relay.at[i2], e_send.at[2], r_recv.at[i2], (t, 0, r))

        def multiply(ref, row, m, slot, first=False, last=False):
            rs = pl.ds(row, m)
            up = jnp.concatenate(
                [
                    jnp.concatenate([wv[QS * slot + q, k % 2, k // 2, 0] for q in range(QS)], axis=1)
                    for k in range(4)
                ],
                axis=0,
            )
            u = gelu(jnp.dot(ref[rs, :], up, preferred_element_type=F32)).astype(BF)
            for k in range(4):
                down = jnp.concatenate(
                    [
                        jnp.concatenate(
                            [
                                wv[QS * slot + q, k % 2, k // 2, 1, j * 128 : (j + 1) * 128, :]
                                for q in range(QS)
                            ],
                            axis=0,
                        )
                        for j in range(4)
                    ],
                    axis=1,
                )
                cs = pl.ds(k * 512, 512)
                part = jnp.dot(u, down, preferred_element_type=F32)
                if last:
                    ref[rs, cs] = (ref[rs, cs].astype(F32) + (acc[rs, cs] + part)).astype(BF)
                elif first:
                    acc[rs, cs] = part
                else:
                    acc[rs, cs] += part

        def step1(sp, _):
            slot = lax.rem(sp, 2)
            loaded(slot)

            def block(i, _):
                row = pl.multiple_of(i * M1, M1)
                tick(QS * sp + i)

                @pl.when(sp < NST - 1)
                def _():
                    multiply(h, row, M1, slot)

                @pl.when(sp == NST - 1)
                def _():
                    load(i, i)

                    @pl.when(i > 0)
                    def _():
                        wait(h.at[pl.ds(0, M1)], o_sem)
                        give(i - 1)

                    multiply(h, row, M1, slot, last=True)
                    store(h, row, M1, pl.multiple_of(base + i * M1, M1)).start()

                return 0

            lax.fori_loop(0, R1 // M1, block, 0)
            return 0

        lax.fori_loop(0, NST, step1, 0)
        second.wait()
        loaded(0)
        for q in range(QS):
            load(QS + q, QS + q)
        for i in range(R2 // M2):
            multiply(h2, i * M2, M2, 0, first=True)
            if i == 0:
                wait(h.at[pl.ds(0, M1)], o_sem)
                give(R1 // M1 - 1)

        def step2(sp, _):
            slot = lax.rem(sp, 2)
            loaded(slot)

            @pl.when(sp < NST - 1)
            def _():
                for q in range(QS):
                    load(QS * (sp + 1) + q, QS * (1 - slot) + q)

            def block(i, _):
                row = pl.multiple_of(i * M2, M2)

                @pl.when(sp < NST - 1)
                def _():
                    multiply(h2, row, M2, slot)

                @pl.when(sp == NST - 1)
                def _():
                    multiply(h2, row, M2, slot, last=True)
                    store(h2, row, M2, pl.multiple_of(2 * R1 + i * M2, M2)).start()

                return 0

            lax.fori_loop(0, R2 // M2, block, 0)
            return 0

        lax.fori_loop(1, NST, step2, 0)
        wait(h2, o_sem)

        half_rows = out.at[pl.ds(0, R1 // 2)]
        wait(half_rows, e_recv.at[0])
        wait(half_rows, e_recv.at[1])

        @pl.when(t < 3)
        def _():
            wait(half_rows, e_send.at[0])

        @pl.when(t > 0)
        def _():
            wait(half_rows, e_send.at[1])

        @pl.when(jnp.logical_or(t == 1, t == 2))
        def _():
            wait(half_rows, e_send.at[2])

        wait(amount(8 * NCH), s_over)
        wait(amount(4 * (N_A + N_B)), s_opp)
        for tt in range(4):

            @pl.when(t == tt)
            def _():
                if tt < 3:
                    wait(amount((tt + 1) * N_B), s_z.at[0, 0])
                    wait(amount((tt + 1) * 2 * N_G), s_z.at[0, 1])
                if tt > 0:
                    wait(amount((4 - tt) * N_B), s_z.at[1, 0])
                    wait(amount((4 - tt) * 2 * N_G), s_z.at[1, 1])


CR, RING = 512, 8


def finalize_kernel(
    rate, wu_in, gu_in, wd_in, gd_in, res, up_out, dn_out, out, buf, zero, zt, ub, un, r_sem, w_sem, u_sem, v_sem
):
    side = lax.axis_index("side")

    def copy(src, dst, sem):
        return pltpu.make_async_copy(src, dst, sem)

    @pl.when(side == 1)
    def _():
        def read(i):
            return copy(res.at[pl.ds(i * CR, CR)], buf.at[i % RING], r_sem.at[i % RING])

        def write(i):
            return copy(buf.at[i % RING], out.at[pl.ds(i * CR, CR)], w_sem.at[i % RING])

        n = TOK // CR
        for i in range(RING // 2):
            read(i).start()
        zero[...] = jnp.zeros_like(zero)
        for i in range(8):
            copy(zero.at[pl.ds(0, 128)], up_out.at[:, pl.ds(i * 1024, 1024)], u_sem.at[0, 0]).start()
            copy(zero.at[:, pl.ds(0, 128)], dn_out.at[pl.ds(i * 1024, 1024)], u_sem.at[0, 1]).start()
        for i in range(n):
            if i + RING // 2 < n:
                if i >= RING // 2:
                    write(i - RING // 2).wait()
                read(i + RING // 2).start()
            read(i).wait()
            write(i).start()
        for i in range(n - RING, n):
            write(i).wait()
        copy(up_out, up_out, u_sem.at[0, 0]).wait()
        copy(dn_out, dn_out, u_sem.at[0, 1]).wait()

    @pl.when(side == 0)
    def _():
        w = QS * FC

        def parts(g, s):
            f = pl.ds(pl.multiple_of(g * w, w), w)
            return (
                copy(wu_in.at[:, f], ub.at[s, 0], u_sem.at[s, 0]),
                copy(gu_in.at[:, f], ub.at[s, 1], u_sem.at[s, 1]),
                copy(wd_in.at[f, :], un.at[s, 0], u_sem.at[s, 2]),
                copy(gd_in.at[f, :], un.at[s, 1], u_sem.at[s, 3]),
            )

        def back(g, s):
            f = pl.ds(pl.multiple_of(g * w, w), w)
            return (
                copy(ub.at[s, 2], up_out.at[:, f], v_sem.at[s, 0]),
                copy(un.at[s, 2], dn_out.at[f, :], v_sem.at[s, 1]),
            )

        for cp in parts(0, 0) + parts(1, 1):
            cp.start()
        zt[...] = jnp.zeros_like(zt)
        for i in range(TOK // CR):
            copy(zt, out.at[pl.ds(i * CR, CR)], w_sem.at[0]).start()
        lr = rate[0]

        def group(g, _):
            s = lax.rem(g, 2)
            for cp in parts(g, s):
                cp.wait()

            @pl.when(g >= 2)
            def _():
                for cp in back(g - 2, s):
                    cp.wait()

            ub[s, 2] = ub[s, 0] - lr * ub[s, 1]
            un[s, 2] = un[s, 0] - lr * un[s, 1]
            for cp in back(g, s):
                cp.start()

            @pl.when(g + 2 < NST)
            def _():
                for cp in parts(g + 2, s):
                    cp.start()

            return 0

        lax.fori_loop(0, NST, group, 0)
        for s in range(2):
            for cp in back(NST - 2 + s, s):
                cp.wait()
        copy(out, out, w_sem.at[0]).wait()


def finalize(rate, wu, gu, wd, gd, res):
    dma = pltpu.SemaphoreType.DMA
    any_ = pl.BlockSpec(memory_space=pl.ANY)
    return pl.pallas_call(
        finalize_kernel,
        out_shape=(
            jax.ShapeDtypeStruct((128, F), F32),
            jax.ShapeDtypeStruct((F, 128), F32),
            jax.ShapeDtypeStruct((TOK, D), BF),
        ),
        in_specs=[pl.BlockSpec(memory_space=pltpu.SMEM)] + [any_] * 5,
        out_specs=(any_,) * 3,
        scratch_shapes=[
            pltpu.VMEM((RING, CR, D), BF),
            pltpu.VMEM((1024, 1024), F32),
            pltpu.VMEM((CR, D), BF),
            pltpu.VMEM((2, 3, 128, QS * FC), F32),
            pltpu.VMEM((2, 3, QS * FC, 128), F32),
            dma((RING,)), dma((RING,)), dma((2, 4)), dma((2, 2)),
        ],
        compiler_params=pltpu.CompilerParams(vmem_limit_bytes=60 << 20),
        name="finalize",
    )(rate, wu, gu, wd, gd, res)


def sync_and_run(rate, wu, gu, wd, gd, rows):
    dma = pltpu.SemaphoreType.DMA
    any_ = pl.BlockSpec(memory_space=pl.ANY)
    out, _, _ = pl.pallas_call(
        kernel,
        out_shape=(
            jax.ShapeDtypeStruct((TOK, D), BF),
            jax.ShapeDtypeStruct((NCH, 2, 2, 2, 512, FC), BF),
            jax.ShapeDtypeStruct((NPC // 2, PC, D), BF),
        ),
        in_specs=[pl.BlockSpec(memory_space=pltpu.SMEM)] + [any_] * 5,
        out_specs=(any_,) * 3,
        scratch_shapes=[
            pltpu.VMEM((R1, D), BF),
            pltpu.VMEM((R2, D), BF),
            pltpu.VMEM((R1, D), F32),
            pltpu.VMEM((2 * QS, 2, 2, 2, 512, FC), BF),
            dma((NCH,)), dma((NCH,)), dma((NCH, 4)), dma((NCH,)),
            dma(()), dma(()), dma((2,)), dma((2, 2)),
            dma((2 * QS,)), dma((2, 4)), dma((2,)), dma(()),
            dma((2,)), dma((3,)), dma((NPC // 2,)),
        ],
        compiler_params=pltpu.CompilerParams(
            has_side_effects=True, vmem_limit_bytes=67043328
        ),
        name="sync_and_run",
    )(rate, wu, gu, wd, gd, rows)
    return out


def solution(mesh):
    up_spec = P("side", None, ("rep", "tp"), None)
    down_spec = P("side", None, None, ("rep", "tp"))
    tok_spec = P("side", "rep", None, None)

    def device_step(w_up, w_down, g_up, g_down, learn_rate, prompts):
        weights = (learn_rate, w_up[0, 0], g_up[0, 0], w_down[0, 0], g_down[0, 0])
        res = sync_and_run(*weights, prompts[0, 0])
        new_up, new_down, out = finalize(*weights, res)
        return new_up[None, None], new_down[None, None], out[None, None]

    return jax.shard_map(
        device_step,
        mesh=mesh,
        in_specs=(up_spec, down_spec, up_spec, down_spec, P("side"), tok_spec),
        out_specs=(up_spec, down_spec, tok_spec),
        check_vma=False,
    )
```

```python
import functools
import math

import jax
import jax.numpy as jnp
from jax import lax
from jax.experimental import pallas as pl
from jax.experimental.pallas import tpu as pltpu
from jax.sharding import PartitionSpec as P

BF, F32 = jnp.bfloat16, jnp.float32
MESH = pl.DeviceIdType.MESH
D, F, TOK = 2048, 8192, 8192
FC = 128
NCH = F // FC
QS = 4
NST = NCH // QS
M1 = 800
R1 = QS * M1
R2 = TOK - 2 * R1
M2 = R2 // 2
PC = 80
NPC = R1 // PC
N_A, N_B, MUL, OFF = 29, 12, 23, 17
N_G = NCH - N_A - N_B
LEAD = 13
YA, YZ, HOPS, OPP, DONE = 5, 0, (2, 4, 6), 8, 9
T_AHEAD = 3


def gelu(a):
    k = math.sqrt(2.0 / math.pi)
    half = 0.5 * a
    return half + half * jnp.tanh(a * (k + (k * 0.044715) * (a * a)))


def kernel(
    rate, wu_in, gu_in, wd_in, gd_in, rows_in, out, w_all, relay, h, h2, acc, wv,
    y_sem, x_sem, b_sem, d_sem, s_over, s_opp, s_y, s_z, ld_sem, up_sem, h_sem, o_sem,
    e_recv, e_send, r_recv,
):
    t, side, r = lax.axis_index("tp"), lax.axis_index("side"), lax.axis_index("rep")
    x, c = r // 2, r % 2

    def send(src, dst, send_sem, recv_sem, device):
        pltpu.make_async_remote_copy(
            src, dst, send_sem, recv_sem, device_id=device, device_id_type=MESH
        ).start()

    def wait(ref, sem):
        pltpu.make_async_copy(ref, ref, sem).wait()

    def kind(i, late):
        ch = jnp.clip(i - late, 0, NCH - 1)
        real = jnp.logical_and(i >= late, i < NCH + late)
        m = lax.rem((ch + OFF) * MUL, NCH)
        is_a = jnp.logical_and(real, m < N_A)
        is_g = jnp.logical_and(real, m >= N_A + N_B)
        not_a = jnp.logical_and(real, m >= N_A)
        return ch, is_a, jnp.logical_and(not_a, m < N_A + N_B), is_g, not_a

    def band(ch, col, j):
        return w_all.at[ch, c, col, :, pl.ds(j * 128, 128), :]

    def band2(ch, j):
        return w_all.at[ch, c, :, :, pl.ds(j * 128, 128), :]

    def amount(n):
        return out.at[pl.ds(0, 16 * n)]

    barrier = pltpu.get_barrier_semaphore()

    def greet(device):
        pl.semaphore_signal(barrier, inc=1, device_id=device, device_id_type=MESH)

    def greet_all(me):
        greet((t, 1 - me, r))
        greet((t, me, r ^ 2))

        @pl.when(t < 3)
        def _():
            greet((t + 1, me, r))

        @pl.when(t > 0)
        def _():
            greet((t - 1, me, r))

        for relay_t, end_t in ((1, 0), (2, 3)):

            @pl.when(t == (end_t if me else relay_t))
            def _():
                greet((relay_t if me else end_t, 1 - me, r))

    @pl.when(side == 0)
    def _():
        greet_all(0)

        def parts(g):
            s = g % 2
            f0 = pl.multiple_of(g * QS * FC, QS * FC)
            cols, rows = pl.ds(f0, QS * FC), pl.ds(f0, QS * FC)
            up, dn = pl.ds(128 * s, 128), pl.ds(512 + 512 * s, 512)
            return [
                pltpu.make_async_copy(src, dst, up_sem.at[s, k])
                for k, (src, dst) in enumerate(
                    (
                        (wu_in.at[:, cols], acc.at[up, pl.ds(0, 512)]),
                        (gu_in.at[:, cols], acc.at[up, pl.ds(512, 512)]),
                        (wd_in.at[rows, :], acc.at[dn, pl.ds(0, 128)]),
                        (gd_in.at[rows, :], acc.at[dn, pl.ds(128, 128)]),
                    )
                )
            ]

        def update(g):
            s = g % 2
            for cp in parts(g):
                cp.wait()

            @pl.when(g + 1 < NST)
            def _():
                for cp in parts(g + 1):
                    cp.start()

            lr = rate[0]
            up = pl.ds(pl.multiple_of(128 * s, 128), 128)
            new_up = (acc[up, 0:512] - lr * acc[up, 512:1024]).astype(BF)
            for q in range(QS):
                wv[QS * s + q, 0, 0, 0, 0:128, :] = new_up[:, q * FC : (q + 1) * FC]
                dn = pl.ds(pl.multiple_of(512 + 512 * s + q * FC, FC), FC)
                new_dn = (acc[dn, 0:128] - lr * acc[dn, 128:256]).astype(BF)
                wv[QS * s + q, 0, 0, 1, 0:128, :] = new_dn
            cp = pltpu.make_async_copy(
                wv.at[pl.ds(QS * s, QS), 0, 0, :, pl.ds(0, 128), :],
                w_all.at[pl.ds(QS * g, QS), c, x, :, pl.ds(t * 128, 128), :],
                o_sem,
            )
            cp.start()
            cp.wait()

        def along(ch, j, right):
            if right:
                send(band(ch, x, j), band(ch, x, j), s_z.at[0, 0], b_sem.at[ch, j], (t + 1, 0, r))
            else:
                send(band(ch, x, j), band(ch, x, j), s_z.at[1, 0], b_sem.at[ch, j], (t - 1, 0, r))

        def across(ch, col, j, k):
            send(band(ch, col, j), band(ch, col, j), s_y.at[k], y_sem.at[ch], (t, 1, r))

        def own_a(i, late):
            ch, is_a, _, _, _ = kind(i, late)

            @pl.when(is_a)
            def _():
                across(ch, x, t, 0)

                @pl.when(t < 3)
                def _():
                    along(ch, t, True)

                @pl.when(t > 0)
                def _():
                    along(ch, t, False)

        def own_z(i):
            ch, _, _, is_g, not_a = kind(i, 0)

            @pl.when(not_a)
            def _():
                across(ch, x, t, 1)

            @pl.when(is_g)
            def _():
                send(band(ch, x, t), band(ch, x, t), s_opp, x_sem.at[ch], (t, 0, r ^ 2))

        def from_opp(i):
            ch, _, _, is_g, _ = kind(i, 0)

            @pl.when(is_g)
            def _():
                wait(amount(1), x_sem.at[ch])
                across(ch, 1 - x, t, 1)

        def hop(i, late, k):
            ch, is_a, _, _, _ = kind(i, late)

            @pl.when(jnp.logical_and(is_a, t >= k))
            def _():
                wait(amount(1), b_sem.at[ch, t - k])
                across(ch, x, t - k, 0)

                @pl.when(t < 3)
                def _():
                    along(ch, t - k, True)

            @pl.when(jnp.logical_and(is_a, t + k <= 3))
            def _():
                wait(amount(1), b_sem.at[ch, t + k])
                across(ch, x, t + k, 0)

                @pl.when(t > 0)
                def _():
                    along(ch, t + k, False)

        for cp in parts(0):
            cp.start()

        def slot(i, _):
            @pl.when(jnp.logical_and(lax.rem(i, QS) == 0, i < NCH))
            def _():
                update(lax.div(i, QS))

            @pl.when(jnp.logical_and(i == 0, jnp.logical_or(t == 1, t == 2)))
            def _():
                pl.semaphore_wait(barrier, 5)

            @pl.when(jnp.logical_and(i == 0, jnp.logical_or(t == 0, t == 3)))
            def _():
                pl.semaphore_wait(barrier, 3)

            own_a(i, T_AHEAD)
            own_z(i)
            for k in (1, 2, 3):
                hop(i, T_AHEAD + k, k)
            from_opp(i)
            return 0

        lax.fori_loop(0, NCH + T_AHEAD + 3, slot, 0)

        @pl.when(jnp.logical_or(t == 1, t == 2))
        def _():
            base = jnp.where(t == 1, R1, 0)
            end = jnp.where(t == 1, 0, 3)
            odd = t - 1

            def piece(i, _):
                wait(relay.at[i], r_recv.at[i])
                row = pl.multiple_of(base + (2 * i + odd) * PC, PC)
                send(relay.at[i], out.at[pl.ds(row, PC)], e_send.at[2], e_recv.at[odd], (end, 1, r))
                return 0

            lax.fori_loop(0, NPC // 2, piece, 0)
            wait(relay, e_send.at[2])

        wait(amount(4 * N_A), s_y.at[0])
        wait(amount(N_B + 2 * N_G), s_y.at[1])
        wait(amount(N_G), s_opp)
        for tt in range(4):

            @pl.when(t == tt)
            def _():
                if tt < 3:
                    wait(amount((tt + 1) * N_A), s_z.at[0, 0])
                if tt > 0:
                    wait(amount((4 - tt) * N_A), s_z.at[1, 0])


    @pl.when(side == 1)
    def _():
        sib, opp = (t, 1, r ^ 1), (t, 1, r ^ 2)
        greet_all(1)
        greet(sib)
        base = jnp.where(t % 2 == 0, 0, R1)

        def over(ref, ch):
            send(ref, ref, s_over, d_sem.at[ch], sib)

        def along(ch, j, right, is_b, is_g):
            k = 0 if right else 1
            dev = (t + 1, 1, r) if right else (t - 1, 1, r)

            @pl.when(is_b)
            def _():
                send(band(ch, x, j), band(ch, x, j), s_z.at[k, 0], b_sem.at[ch, j], dev)

            @pl.when(is_g)
            def _():
                send(band2(ch, j), band2(ch, j), s_z.at[k, 1], b_sem.at[ch, j], dev)

        def arrive(sem, is_b, is_g):
            @pl.when(is_b)
            def _():
                wait(amount(1), sem)

            @pl.when(is_g)
            def _():
                wait(amount(2), sem)

        def across(ch):
            own = w_all.at[ch, c, x]
            send(own, own, s_opp, x_sem.at[ch], opp)
            over(own, ch)

        def ya(i):
            ch, is_a, _, _, _ = kind(i, YA)

            @pl.when(is_a)
            def _():
                wait(amount(4), y_sem.at[ch])
                across(ch)

        def yz(i):
            ch, _, is_b, is_g, not_a = kind(i, YZ)

            @pl.when(not_a)
            def _():
                arrive(y_sem.at[ch], is_b, is_g)

                @pl.when(t < 3)
                def _():
                    along(ch, t, True, is_b, is_g)

                @pl.when(t > 0)
                def _():
                    along(ch, t, False, is_b, is_g)

        def hop(i, k):
            ch, _, is_b, is_g, not_a = kind(i, HOPS[k - 1])

            @pl.when(jnp.logical_and(not_a, t >= k))
            def _():
                arrive(b_sem.at[ch, t - k], is_b, is_g)

                @pl.when(t < 3)
                def _():
                    along(ch, t - k, True, is_b, is_g)

            @pl.when(jnp.logical_and(not_a, t + k <= 3))
            def _():
                arrive(b_sem.at[ch, t + k], is_b, is_g)

                @pl.when(t > 0)
                def _():
                    along(ch, t + k, False, is_b, is_g)

            if k == 3:

                @pl.when(is_b)
                def _():
                    across(ch)

                @pl.when(is_g)
                def _():
                    over(w_all.at[ch, c], ch)

        def from_opp(i):
            ch, is_a, is_b, _, _ = kind(i, OPP)

            @pl.when(jnp.logical_or(is_a, is_b))
            def _():
                wait(amount(4), x_sem.at[ch])
                over(w_all.at[ch, c, 1 - x], ch)

        def load(ch, ring):
            pltpu.make_async_copy(w_all.at[ch], wv.at[ring], ld_sem.at[ring]).start()

        def ready(i):
            @pl.when(jnp.logical_and(i >= DONE, i < NCH + DONE))
            def _():
                ch = jnp.clip(i - DONE, 0, NCH - 1)
                wait(amount(8), d_sem.at[ch])
                load(ch, lax.rem(ch, 2 * QS))

        def tick(i):
            ya(i)
            hop(i, 3)
            from_opp(i)
            hop(i, 2)
            yz(i)
            hop(i, 1)
            ready(i)

        def loaded(slot):
            for q in range(QS):
                wait(wv.at[QS * slot + q], ld_sem.at[QS * slot + q])

        def store(ref, row, n, to):
            return pltpu.make_async_copy(ref.at[pl.ds(row, n)], out.at[pl.ds(to, n)], o_sem)

        first = pltpu.make_async_copy(
            rows_in.at[pl.ds(pl.multiple_of(base, 128), R1)], h, h_sem.at[0]
        )
        second = pltpu.make_async_copy(rows_in.at[pl.ds(2 * R1, R2)], h2, h_sem.at[1])
        first.start()
        second.start()

        def zero(i, _):
            acc[pl.ds(pl.multiple_of(i * 128, 128), 128), :] = jnp.zeros((128, D), F32)
            return 0

        lax.fori_loop(0, R1 // 128, zero, 0)
        first.wait()
        pl.semaphore_wait(barrier, 5)
        lax.fori_loop(0, LEAD, lambda i, _: (tick(i), 0)[1], 0)

        def give(i):
            for q in range(M1 // PC):
                p = i * (M1 // PC) + q
                src = out.at[pl.ds(pl.multiple_of(base + p * PC, PC), PC)]
                i2 = i * (M1 // PC // 2) + q // 2
                if q % 2 == 0:

                    @pl.when(t < 3)
                    def _():
                        send(src, src, e_send.at[0], e_recv.at[0], (t + 1, 1, r))

                    @pl.when(t == 1)
                    def _():
                        send(src, relay.at[i2], e_send.at[2], r_recv.at[i2], (t, 0, r))
                else:

                    @pl.when(t > 0)
                    def _():
                        send(src, src, e_send.at[1], e_recv.at[1], (t - 1, 1, r))

                    @pl.when(t == 2)
                    def _():
                        send(src, relay.at[i2], e_send.at[2], r_recv.at[i2], (t, 0, r))

        def multiply(ref, row, m, slot, first=False, last=False):
            rs = pl.ds(row, m)
            up = jnp.concatenate(
                [
                    jnp.concatenate([wv[QS * slot + q, k % 2, k // 2, 0] for q in range(QS)], axis=1)
                    for k in range(4)
                ],
                axis=0,
            )
            u = gelu(jnp.dot(ref[rs, :], up, preferred_element_type=F32)).astype(BF)
            for k in range(4):
                down = jnp.concatenate(
                    [
                        jnp.concatenate(
                            [
                                wv[QS * slot + q, k % 2, k // 2, 1, j * 128 : (j + 1) * 128, :]
                                for q in range(QS)
                            ],
                            axis=0,
                        )
                        for j in range(4)
                    ],
                    axis=1,
                )
                cs = pl.ds(k * 512, 512)
                part = jnp.dot(u, down, preferred_element_type=F32)
                if last:
                    ref[rs, cs] = (ref[rs, cs].astype(F32) + (acc[rs, cs] + part)).astype(BF)
                elif first:
                    acc[rs, cs] = part
                else:
                    acc[rs, cs] += part

        def step1(sp, _):
            slot = lax.rem(sp, 2)
            loaded(slot)

            def block(i, _):
                row = pl.multiple_of(i * M1, M1)
                tick(LEAD + QS * sp + i)

                @pl.when(sp < NST - 1)
                def _():
                    multiply(h, row, M1, slot)

                @pl.when(sp == NST - 1)
                def _():
                    load(i, i)

                    @pl.when(i > 0)
                    def _():
                        wait(h.at[pl.ds(0, M1)], o_sem)
                        give(i - 1)

                    multiply(h, row, M1, slot, last=True)
                    store(h, row, M1, pl.multiple_of(base + i * M1, M1)).start()

                return 0

            lax.fori_loop(0, R1 // M1, block, 0)
            return 0

        lax.fori_loop(0, NST, step1, 0)
        second.wait()
        loaded(0)
        for q in range(QS):
            load(QS + q, QS + q)
        for i in range(R2 // M2):
            multiply(h2, i * M2, M2, 0, first=True)
            if i == 0:
                wait(h.at[pl.ds(0, M1)], o_sem)
                give(R1 // M1 - 1)

        def step2(sp, _):
            slot = lax.rem(sp, 2)
            loaded(slot)

            @pl.when(sp < NST - 1)
            def _():
                for q in range(QS):
                    load(QS * (sp + 1) + q, QS * (1 - slot) + q)

            def block(i, _):
                row = pl.multiple_of(i * M2, M2)

                @pl.when(sp < NST - 1)
                def _():
                    multiply(h2, row, M2, slot)

                @pl.when(sp == NST - 1)
                def _():
                    multiply(h2, row, M2, slot, last=True)
                    store(h2, row, M2, pl.multiple_of(2 * R1 + i * M2, 128)).start()

                return 0

            lax.fori_loop(0, R2 // M2, block, 0)
            return 0

        lax.fori_loop(1, NST, step2, 0)
        wait(h2, o_sem)

        half_rows = out.at[pl.ds(0, R1 // 2)]
        wait(half_rows, e_recv.at[0])
        wait(half_rows, e_recv.at[1])

        @pl.when(t < 3)
        def _():
            wait(half_rows, e_send.at[0])

        @pl.when(t > 0)
        def _():
            wait(half_rows, e_send.at[1])

        @pl.when(jnp.logical_or(t == 1, t == 2))
        def _():
            wait(half_rows, e_send.at[2])

        wait(amount(8 * NCH), s_over)
        wait(amount(4 * (N_A + N_B)), s_opp)
        for tt in range(4):

            @pl.when(t == tt)
            def _():
                if tt < 3:
                    wait(amount((tt + 1) * N_B), s_z.at[0, 0])
                    wait(amount((tt + 1) * 2 * N_G), s_z.at[0, 1])
                if tt > 0:
                    wait(amount((4 - tt) * N_B), s_z.at[1, 0])
                    wait(amount((4 - tt) * 2 * N_G), s_z.at[1, 1])


CR, RING = 512, 8


def finalize_kernel(
    rate, wu_in, gu_in, wd_in, gd_in, res, up_out, dn_out, out, buf, zero, zt, ub, un, r_sem, w_sem, u_sem, v_sem
):
    side = lax.axis_index("side")

    def copy(src, dst, sem):
        return pltpu.make_async_copy(src, dst, sem)

    @pl.when(side == 1)
    def _():
        def read(i):
            return copy(res.at[pl.ds(i * CR, CR)], buf.at[i % RING], r_sem.at[i % RING])

        def write(i):
            return copy(buf.at[i % RING], out.at[pl.ds(i * CR, CR)], w_sem.at[i % RING])

        n = TOK // CR
        for i in range(RING // 2):
            read(i).start()
        zero[...] = jnp.zeros_like(zero)
        for i in range(8):
            copy(zero.at[pl.ds(0, 128)], up_out.at[:, pl.ds(i * 1024, 1024)], u_sem.at[0, 0]).start()
            copy(zero.at[:, pl.ds(0, 128)], dn_out.at[pl.ds(i * 1024, 1024)], u_sem.at[0, 1]).start()
        for i in range(n):
            if i + RING // 2 < n:
                if i >= RING // 2:
                    write(i - RING // 2).wait()
                read(i + RING // 2).start()
            read(i).wait()
            write(i).start()
        for i in range(n - RING, n):
            write(i).wait()
        copy(up_out, up_out, u_sem.at[0, 0]).wait()
        copy(dn_out, dn_out, u_sem.at[0, 1]).wait()

    @pl.when(side == 0)
    def _():
        w = QS * FC

        def parts(g, s):
            f = pl.ds(pl.multiple_of(g * w, w), w)
            return (
                copy(wu_in.at[:, f], ub.at[s, 0], u_sem.at[s, 0]),
                copy(gu_in.at[:, f], ub.at[s, 1], u_sem.at[s, 1]),
                copy(wd_in.at[f, :], un.at[s, 0], u_sem.at[s, 2]),
                copy(gd_in.at[f, :], un.at[s, 1], u_sem.at[s, 3]),
            )

        def back(g, s):
            f = pl.ds(pl.multiple_of(g * w, w), w)
            return (
                copy(ub.at[s, 2], up_out.at[:, f], v_sem.at[s, 0]),
                copy(un.at[s, 2], dn_out.at[f, :], v_sem.at[s, 1]),
            )

        for cp in parts(0, 0) + parts(1, 1):
            cp.start()
        zt[...] = jnp.zeros_like(zt)
        for i in range(TOK // CR):
            copy(zt, out.at[pl.ds(i * CR, CR)], w_sem.at[0]).start()
        lr = rate[0]

        def group(g, _):
            s = lax.rem(g, 2)
            for cp in parts(g, s):
                cp.wait()

            @pl.when(g >= 2)
            def _():
                for cp in back(g - 2, s):
                    cp.wait()

            ub[s, 2] = ub[s, 0] - lr * ub[s, 1]
            un[s, 2] = un[s, 0] - lr * un[s, 1]
            for cp in back(g, s):
                cp.start()

            @pl.when(g + 2 < NST)
            def _():
                for cp in parts(g + 2, s):
                    cp.start()

            return 0

        lax.fori_loop(0, NST, group, 0)
        for s in range(2):
            for cp in back(NST - 2 + s, s):
                cp.wait()
        copy(out, out, w_sem.at[0]).wait()


def finalize(rate, wu, gu, wd, gd, res):
    dma = pltpu.SemaphoreType.DMA
    any_ = pl.BlockSpec(memory_space=pl.ANY)
    return pl.pallas_call(
        finalize_kernel,
        out_shape=(
            jax.ShapeDtypeStruct((128, F), F32),
            jax.ShapeDtypeStruct((F, 128), F32),
            jax.ShapeDtypeStruct((TOK, D), BF),
        ),
        in_specs=[pl.BlockSpec(memory_space=pltpu.SMEM)] + [any_] * 5,
        out_specs=(any_,) * 3,
        scratch_shapes=[
            pltpu.VMEM((RING, CR, D), BF),
            pltpu.VMEM((1024, 1024), F32),
            pltpu.VMEM((CR, D), BF),
            pltpu.VMEM((2, 3, 128, QS * FC), F32),
            pltpu.VMEM((2, 3, QS * FC, 128), F32),
            dma((RING,)), dma((RING,)), dma((2, 4)), dma((2, 2)),
        ],
        compiler_params=pltpu.CompilerParams(vmem_limit_bytes=60 << 20),
        name="finalize",
    )(rate, wu, gu, wd, gd, res)


def sync_and_run(rate, wu, gu, wd, gd, rows):
    dma = pltpu.SemaphoreType.DMA
    any_ = pl.BlockSpec(memory_space=pl.ANY)
    out, _, _ = pl.pallas_call(
        kernel,
        out_shape=(
            jax.ShapeDtypeStruct((TOK, D), BF),
            jax.ShapeDtypeStruct((NCH, 2, 2, 2, 512, FC), BF),
            jax.ShapeDtypeStruct((NPC // 2, PC, D), BF),
        ),
        in_specs=[pl.BlockSpec(memory_space=pltpu.SMEM)] + [any_] * 5,
        out_specs=(any_,) * 3,
        scratch_shapes=[
            pltpu.VMEM((R1, D), BF),
            pltpu.VMEM((R2, D), BF),
            pltpu.VMEM((R1, D), F32),
            pltpu.VMEM((2 * QS, 2, 2, 2, 512, FC), BF),
            dma((NCH,)), dma((NCH,)), dma((NCH, 4)), dma((NCH,)),
            dma(()), dma(()), dma((2,)), dma((2, 2)),
            dma((2 * QS,)), dma((2, 4)), dma((2,)), dma(()),
            dma((2,)), dma((3,)), dma((NPC // 2,)),
        ],
        compiler_params=pltpu.CompilerParams(
            has_side_effects=True, vmem_limit_bytes=67043328, collective_id=0
        ),
        name="sync_and_run",
    )(rate, wu, gu, wd, gd, rows)
    return out


def solution(mesh):
    up_spec = P("side", None, ("rep", "tp"), None)
    down_spec = P("side", None, None, ("rep", "tp"))
    tok_spec = P("side", "rep", None, None)

    def device_step(w_up, w_down, g_up, g_down, learn_rate, prompts):
        weights = (learn_rate, w_up[0, 0], g_up[0, 0], w_down[0, 0], g_down[0, 0])
        res = sync_and_run(*weights, prompts[0, 0])
        new_up, new_down, out = finalize(*weights, res)
        return new_up[None, None], new_down[None, None], out[None, None]

    return jax.shard_map(
        device_step,
        mesh=mesh,
        in_specs=(up_spec, down_spec, up_spec, down_spec, P("side"), tok_spec),
        out_specs=(up_spec, down_spec, tok_spec),
        check_vma=False,
    )
```

```python
import functools
import math

import jax
import jax.numpy as jnp
from jax import lax
from jax.experimental import pallas as pl
from jax.experimental.pallas import tpu as pltpu
from jax.sharding import PartitionSpec as P

BF, F32 = jnp.bfloat16, jnp.float32
MESH = pl.DeviceIdType.MESH
D, F, TOK = 2048, 8192, 8192
FC = 128
NCH = F // FC
QS = 4
NST = NCH // QS
M1 = 800
R1 = QS * M1
R2 = TOK - 2 * R1
M2 = R2 // 2
PC = 40
NPC = R1 // PC
VIA = NPC // 2 - 1
N_A, N_B, MUL, OFF = 29, 12, 23, 17
N_G = NCH - N_A - N_B
LEAD = 13
YA, YZ, HOPS, OPP, DONE = 5, 0, (2, 4, 6), 8, 9
T_AHEAD = 3


def gelu(a):
    k = math.sqrt(2.0 / math.pi)
    half = 0.5 * a
    return half + half * jnp.tanh(a * (k + (k * 0.044715) * (a * a)))


def kernel(
    rate, wu_in, gu_in, wd_in, gd_in, rows_in, out, w_all, relay, h, h2, acc, wv,
    y_sem, x_sem, b_sem, d_sem, s_over, s_opp, s_y, s_z, ld_sem, up_sem, h_sem, o_sem,
    e_recv, e_send, r_recv,
):
    t, side, r = lax.axis_index("tp"), lax.axis_index("side"), lax.axis_index("rep")
    x, c = r // 2, r % 2

    def send(src, dst, send_sem, recv_sem, device):
        pltpu.make_async_remote_copy(
            src, dst, send_sem, recv_sem, device_id=device, device_id_type=MESH
        ).start()

    def wait(ref, sem):
        pltpu.make_async_copy(ref, ref, sem).wait()

    def kind(i, late):
        ch = jnp.clip(i - late, 0, NCH - 1)
        real = jnp.logical_and(i >= late, i < NCH + late)
        m = lax.rem((ch + OFF) * MUL, NCH)
        is_a = jnp.logical_and(real, m < N_A)
        is_g = jnp.logical_and(real, m >= N_A + N_B)
        not_a = jnp.logical_and(real, m >= N_A)
        return ch, is_a, jnp.logical_and(not_a, m < N_A + N_B), is_g, not_a

    def band(ch, col, j):
        return w_all.at[ch, c, col, :, pl.ds(j * 128, 128), :]

    def band2(ch, j):
        return w_all.at[ch, c, :, :, pl.ds(j * 128, 128), :]

    def amount(n):
        return out.at[pl.ds(0, 16 * n)]

    barrier = pltpu.get_barrier_semaphore()

    def greet(device):
        pl.semaphore_signal(barrier, inc=1, device_id=device, device_id_type=MESH)

    def greet_all(me):
        greet((t, 1 - me, r))
        greet((t, me, r ^ 2))

        @pl.when(t < 3)
        def _():
            greet((t + 1, me, r))

        @pl.when(t > 0)
        def _():
            greet((t - 1, me, r))

        for relay_t, end_t in ((1, 0), (2, 3)):

            @pl.when(t == (end_t if me else relay_t))
            def _():
                greet((relay_t if me else end_t, 1 - me, r))

    @pl.when(side == 0)
    def _():
        greet_all(0)

        def parts(g):
            s = g % 2
            f0 = pl.multiple_of(g * QS * FC, QS * FC)
            cols, rows = pl.ds(f0, QS * FC), pl.ds(f0, QS * FC)
            up, dn = pl.ds(128 * s, 128), pl.ds(512 + 512 * s, 512)
            return [
                pltpu.make_async_copy(src, dst, up_sem.at[s, k])
                for k, (src, dst) in enumerate(
                    (
                        (wu_in.at[:, cols], acc.at[up, pl.ds(0, 512)]),
                        (gu_in.at[:, cols], acc.at[up, pl.ds(512, 512)]),
                        (wd_in.at[rows, :], acc.at[dn, pl.ds(0, 128)]),
                        (gd_in.at[rows, :], acc.at[dn, pl.ds(128, 128)]),
                    )
                )
            ]

        def update(g):
            s = g % 2
            for cp in parts(g):
                cp.wait()

            @pl.when(g + 1 < NST)
            def _():
                for cp in parts(g + 1):
                    cp.start()

            lr = rate[0]
            up = pl.ds(pl.multiple_of(128 * s, 128), 128)
            new_up = (acc[up, 0:512] - lr * acc[up, 512:1024]).astype(BF)
            for q in range(QS):
                wv[QS * s + q, 0, 0, 0, 0:128, :] = new_up[:, q * FC : (q + 1) * FC]
                dn = pl.ds(pl.multiple_of(512 + 512 * s + q * FC, FC), FC)
                new_dn = (acc[dn, 0:128] - lr * acc[dn, 128:256]).astype(BF)
                wv[QS * s + q, 0, 0, 1, 0:128, :] = new_dn
            cp = pltpu.make_async_copy(
                wv.at[pl.ds(QS * s, QS), 0, 0, :, pl.ds(0, 128), :],
                w_all.at[pl.ds(QS * g, QS), c, x, :, pl.ds(t * 128, 128), :],
                o_sem,
            )
            cp.start()
            cp.wait()

        def along(ch, j, right):
            if right:
                send(band(ch, x, j), band(ch, x, j), s_z.at[0, 0], b_sem.at[ch, j], (t + 1, 0, r))
            else:
                send(band(ch, x, j), band(ch, x, j), s_z.at[1, 0], b_sem.at[ch, j], (t - 1, 0, r))

        def across(ch, col, j, k):
            send(band(ch, col, j), band(ch, col, j), s_y.at[k], y_sem.at[ch], (t, 1, r))

        def own_a(i, late):
            ch, is_a, _, _, _ = kind(i, late)

            @pl.when(is_a)
            def _():
                across(ch, x, t, 0)

                @pl.when(t < 3)
                def _():
                    along(ch, t, True)

                @pl.when(t > 0)
                def _():
                    along(ch, t, False)

        def own_z(i):
            ch, _, _, is_g, not_a = kind(i, 0)

            @pl.when(not_a)
            def _():
                across(ch, x, t, 1)

            @pl.when(is_g)
            def _():
                send(band(ch, x, t), band(ch, x, t), s_opp, x_sem.at[ch], (t, 0, r ^ 2))

        def from_opp(i):
            ch, _, _, is_g, _ = kind(i, 0)

            @pl.when(is_g)
            def _():
                wait(amount(1), x_sem.at[ch])
                across(ch, 1 - x, t, 1)

        def hop(i, late, k):
            ch, is_a, _, _, _ = kind(i, late)

            @pl.when(jnp.logical_and(is_a, t >= k))
            def _():
                wait(amount(1), b_sem.at[ch, t - k])
                across(ch, x, t - k, 0)

                @pl.when(t < 3)
                def _():
                    along(ch, t - k, True)

            @pl.when(jnp.logical_and(is_a, t + k <= 3))
            def _():
                wait(amount(1), b_sem.at[ch, t + k])
                across(ch, x, t + k, 0)

                @pl.when(t > 0)
                def _():
                    along(ch, t + k, False)

        for cp in parts(0):
            cp.start()

        def slot(i, _):
            @pl.when(jnp.logical_and(lax.rem(i, QS) == 0, i < NCH))
            def _():
                update(lax.div(i, QS))

            @pl.when(jnp.logical_and(i == 0, jnp.logical_or(t == 1, t == 2)))
            def _():
                pl.semaphore_wait(barrier, 5)

            @pl.when(jnp.logical_and(i == 0, jnp.logical_or(t == 0, t == 3)))
            def _():
                pl.semaphore_wait(barrier, 3)

            own_a(i, T_AHEAD)
            own_z(i)
            for k in (1, 2, 3):
                hop(i, T_AHEAD + k, k)
            from_opp(i)
            return 0

        lax.fori_loop(0, NCH + T_AHEAD + 3, slot, 0)

        @pl.when(jnp.logical_or(t == 1, t == 2))
        def _():
            base = jnp.where(t == 1, R1, 0)
            end = jnp.where(t == 1, 0, 3)
            odd = t - 1

            def piece(i, _):
                wait(relay.at[i], r_recv.at[i])
                row = pl.multiple_of(base + (2 * i + odd) * PC, PC)
                send(relay.at[i], out.at[pl.ds(row, PC)], e_send.at[2], e_recv.at[odd], (end, 1, r))
                return 0

            lax.fori_loop(0, VIA, piece, 0)
            wait(relay, e_send.at[2])

        wait(amount(4 * N_A), s_y.at[0])
        wait(amount(N_B + 2 * N_G), s_y.at[1])
        wait(amount(N_G), s_opp)
        for tt in range(4):

            @pl.when(t == tt)
            def _():
                if tt < 3:
                    wait(amount((tt + 1) * N_A), s_z.at[0, 0])
                if tt > 0:
                    wait(amount((4 - tt) * N_A), s_z.at[1, 0])


    @pl.when(side == 1)
    def _():
        sib, opp = (t, 1, r ^ 1), (t, 1, r ^ 2)
        greet_all(1)
        greet(sib)
        base = jnp.where(t % 2 == 0, 0, R1)

        def over(ref, ch):
            send(ref, ref, s_over, d_sem.at[ch], sib)

        def along(ch, j, right, is_b, is_g):
            k = 0 if right else 1
            dev = (t + 1, 1, r) if right else (t - 1, 1, r)

            @pl.when(is_b)
            def _():
                send(band(ch, x, j), band(ch, x, j), s_z.at[k, 0], b_sem.at[ch, j], dev)

            @pl.when(is_g)
            def _():
                send(band2(ch, j), band2(ch, j), s_z.at[k, 1], b_sem.at[ch, j], dev)

        def arrive(sem, is_b, is_g):
            @pl.when(is_b)
            def _():
                wait(amount(1), sem)

            @pl.when(is_g)
            def _():
                wait(amount(2), sem)

        def across(ch):
            own = w_all.at[ch, c, x]
            send(own, own, s_opp, x_sem.at[ch], opp)
            over(own, ch)

        def ya(i):
            ch, is_a, _, _, _ = kind(i, YA)

            @pl.when(is_a)
            def _():
                wait(amount(4), y_sem.at[ch])
                across(ch)

        def yz(i):
            ch, _, is_b, is_g, not_a = kind(i, YZ)

            @pl.when(not_a)
            def _():
                arrive(y_sem.at[ch], is_b, is_g)

                @pl.when(t < 3)
                def _():
                    along(ch, t, True, is_b, is_g)

                @pl.when(t > 0)
                def _():
                    along(ch, t, False, is_b, is_g)

        def hop(i, k):
            ch, _, is_b, is_g, not_a = kind(i, HOPS[k - 1])

            @pl.when(jnp.logical_and(not_a, t >= k))
            def _():
                arrive(b_sem.at[ch, t - k], is_b, is_g)

                @pl.when(t < 3)
                def _():
                    along(ch, t - k, True, is_b, is_g)

            @pl.when(jnp.logical_and(not_a, t + k <= 3))
            def _():
                arrive(b_sem.at[ch, t + k], is_b, is_g)

                @pl.when(t > 0)
                def _():
                    along(ch, t + k, False, is_b, is_g)

            if k == 3:

                @pl.when(is_b)
                def _():
                    across(ch)

                @pl.when(is_g)
                def _():
                    over(w_all.at[ch, c], ch)

        def from_opp(i):
            ch, is_a, is_b, _, _ = kind(i, OPP)

            @pl.when(jnp.logical_or(is_a, is_b))
            def _():
                wait(amount(4), x_sem.at[ch])
                over(w_all.at[ch, c, 1 - x], ch)

        def load(ch, ring):
            pltpu.make_async_copy(w_all.at[ch], wv.at[ring], ld_sem.at[ring]).start()

        def ready(i):
            @pl.when(jnp.logical_and(i >= DONE, i < NCH + DONE))
            def _():
                ch = jnp.clip(i - DONE, 0, NCH - 1)
                wait(amount(8), d_sem.at[ch])
                load(ch, lax.rem(ch, 2 * QS))

        def tick(i):
            ya(i)
            hop(i, 3)
            from_opp(i)
            hop(i, 2)
            yz(i)
            hop(i, 1)
            ready(i)

        def loaded(slot):
            for q in range(QS):
                wait(wv.at[QS * slot + q], ld_sem.at[QS * slot + q])

        first = pltpu.make_async_copy(
            rows_in.at[pl.ds(pl.multiple_of(base, 128), R1)], h, h_sem.at[0]
        )
        second = pltpu.make_async_copy(rows_in.at[pl.ds(2 * R1, R2)], h2, h_sem.at[1])
        first.start()
        second.start()

        def zero(i, _):
            acc[pl.ds(pl.multiple_of(i * 128, 128), 128), :] = jnp.zeros((128, D), F32)
            return 0

        lax.fori_loop(0, R1 // 128, zero, 0)
        first.wait()
        pl.semaphore_wait(barrier, 5)
        lax.fori_loop(0, LEAD, lambda i, _: (tick(i), 0)[1], 0)

        def give(i):
            def pieces(q, _):
                i2 = i * (M1 // PC // 2) + q
                right, left = (t + 1, 1, r), (t - 1, 1, r)
                for odd in range(2):
                    row = pl.multiple_of(base + (2 * i2 + odd) * PC, PC)
                    src = out.at[pl.ds(row, PC)]

                    @pl.when(t > 0 if odd else t < 3)
                    def _():
                        send(src, src, e_send.at[odd], e_recv.at[odd], left if odd else right)

                    @pl.when(jnp.logical_and(t == 1 + odd, i2 < VIA))
                    def _():
                        to = jnp.minimum(i2, VIA - 1)
                        send(src, relay.at[to], e_send.at[2], r_recv.at[to], (t, 0, r))

                    @pl.when(jnp.logical_and(t == 1 + odd, i2 >= VIA))
                    def _():
                        send(src, src, e_send.at[3], e_recv.at[odd], right if odd else left)

                return 0

            lax.fori_loop(0, M1 // PC // 2, pieces, 0)

        def multiply(ref, rows, slot, first=False, last=None):
            up = jnp.concatenate(
                [
                    jnp.concatenate([wv[QS * slot + q, k % 2, k // 2, 0] for q in range(QS)], axis=1)
                    for k in range(4)
                ],
                axis=0,
            )

            def down(k):
                return jnp.concatenate(
                    [
                        jnp.concatenate(
                            [
                                wv[QS * slot + q, k % 2, k // 2, 1, j * 128 : (j + 1) * 128, :]
                                for q in range(QS)
                            ],
                            axis=0,
                        )
                        for j in range(4)
                    ],
                    axis=1,
                )

            pre = jnp.dot(ref[rows[0], :], up, preferred_element_type=F32)
            for n, rs in enumerate(rows):
                if n + 1 < len(rows):
                    ahead = jnp.dot(ref[rows[n + 1], :], up, preferred_element_type=F32)
                u = gelu(pre).astype(BF)
                for k in range(4):
                    cs = pl.ds(k * 512, 512)
                    part = jnp.dot(u, down(k), preferred_element_type=F32)
                    if last is not None:
                        ref[rs, cs] = (ref[rs, cs].astype(F32) + (acc[rs, cs] + part)).astype(BF)
                        to = out.at[pl.ds(last[n], rs.size), cs]
                        pltpu.make_async_copy(ref.at[rs, cs], to, o_sem).start()
                    elif first:
                        acc[rs, cs] = part
                    else:
                        acc[rs, cs] += part
                pre = ahead if n + 1 < len(rows) else None

        def step1(sp, _):
            slot = lax.rem(sp, 2)
            loaded(slot)

            def block(i, _):
                tick(LEAD + QS * sp + i)
                multiply(h, [pl.ds(pl.multiple_of(i * M1, M1), M1)], slot)
                return 0

            lax.fori_loop(0, R1 // M1, block, 0)
            return 0

        lax.fori_loop(0, NST - 1, step1, 0)
        loaded(1)

        def last1(i, _):
            load(i, i)

            @pl.when(i > 0)
            def _():
                wait(h.at[pl.ds(0, M1)], o_sem)
                give(i - 1)

            row = pl.multiple_of(i * M1, M1)
            multiply(h, [pl.ds(row, M1)], 1, last=[pl.multiple_of(base + i * M1, M1)])
            return 0

        lax.fori_loop(0, R1 // M1, last1, 0)
        second.wait()
        loaded(0)
        for q in range(QS):
            load(QS + q, QS + q)
        wait(h.at[pl.ds(0, M1)], o_sem)
        give(R1 // M1 - 1)
        halves = [pl.ds(0, M2), pl.ds(M2, M2)]
        multiply(h2, halves, 0, first=True)

        def step2(sp, _):
            slot = lax.rem(sp, 2)
            loaded(slot)
            for q in range(QS):
                load(QS * (sp + 1) + q, QS * (1 - slot) + q)

            multiply(h2, halves, slot)
            return 0

        lax.fori_loop(1, NST - 1, step2, 0)
        loaded(1)
        multiply(h2, halves, 1, last=[2 * R1, 2 * R1 + M2])
        wait(h2, o_sem)

        half_rows = out.at[pl.ds(0, R1 // 2)]
        wait(half_rows, e_recv.at[0])
        wait(half_rows, e_recv.at[1])

        @pl.when(t < 3)
        def _():
            wait(half_rows, e_send.at[0])

        @pl.when(t > 0)
        def _():
            wait(half_rows, e_send.at[1])

        @pl.when(jnp.logical_or(t == 1, t == 2))
        def _():
            wait(out.at[pl.ds(0, VIA * PC)], e_send.at[2])
            wait(out.at[pl.ds(0, R1 // 2 - VIA * PC)], e_send.at[3])

        wait(amount(8 * NCH), s_over)
        wait(amount(4 * (N_A + N_B)), s_opp)
        for tt in range(4):

            @pl.when(t == tt)
            def _():
                if tt < 3:
                    wait(amount((tt + 1) * N_B), s_z.at[0, 0])
                    wait(amount((tt + 1) * 2 * N_G), s_z.at[0, 1])
                if tt > 0:
                    wait(amount((4 - tt) * N_B), s_z.at[1, 0])
                    wait(amount((4 - tt) * 2 * N_G), s_z.at[1, 1])


CR, RING = 512, 8


def finalize_kernel(
    rate, wu_in, gu_in, wd_in, gd_in, res, up_out, dn_out, out, buf, zero, zt, ub, un, r_sem, w_sem, u_sem, v_sem
):
    side = lax.axis_index("side")

    def copy(src, dst, sem):
        return pltpu.make_async_copy(src, dst, sem)

    @pl.when(side == 1)
    def _():
        def read(i):
            return copy(res.at[pl.ds(i * CR, CR)], buf.at[i % RING], r_sem.at[i % RING])

        def write(i):
            return copy(buf.at[i % RING], out.at[pl.ds(i * CR, CR)], w_sem.at[i % RING])

        n = TOK // CR
        for i in range(RING // 2):
            read(i).start()
        zero[...] = jnp.zeros_like(zero)
        for i in range(8):
            copy(zero.at[pl.ds(0, 128)], up_out.at[:, pl.ds(i * 1024, 1024)], u_sem.at[0, 0]).start()
            copy(zero.at[:, pl.ds(0, 128)], dn_out.at[pl.ds(i * 1024, 1024)], u_sem.at[0, 1]).start()
        for i in range(n):
            if i + RING // 2 < n:
                if i >= RING // 2:
                    write(i - RING // 2).wait()
                read(i + RING // 2).start()
            read(i).wait()
            write(i).start()
        for i in range(n - RING, n):
            write(i).wait()
        copy(up_out, up_out, u_sem.at[0, 0]).wait()
        copy(dn_out, dn_out, u_sem.at[0, 1]).wait()

    @pl.when(side == 0)
    def _():
        w = QS * FC

        def parts(g, s):
            f = pl.ds(pl.multiple_of(g * w, w), w)
            return (
                copy(wu_in.at[:, f], ub.at[s, 0], u_sem.at[s, 0]),
                copy(gu_in.at[:, f], ub.at[s, 1], u_sem.at[s, 1]),
                copy(wd_in.at[f, :], un.at[s, 0], u_sem.at[s, 2]),
                copy(gd_in.at[f, :], un.at[s, 1], u_sem.at[s, 3]),
            )

        def back(g, s):
            f = pl.ds(pl.multiple_of(g * w, w), w)
            return (
                copy(ub.at[s, 2], up_out.at[:, f], v_sem.at[s, 0]),
                copy(un.at[s, 2], dn_out.at[f, :], v_sem.at[s, 1]),
            )

        for cp in parts(0, 0) + parts(1, 1):
            cp.start()
        zt[...] = jnp.zeros_like(zt)
        for i in range(TOK // CR):
            copy(zt, out.at[pl.ds(i * CR, CR)], w_sem.at[0]).start()
        lr = rate[0]

        def group(g, _):
            s = lax.rem(g, 2)
            for cp in parts(g, s):
                cp.wait()

            @pl.when(g >= 2)
            def _():
                for cp in back(g - 2, s):
                    cp.wait()

            ub[s, 2] = ub[s, 0] - lr * ub[s, 1]
            un[s, 2] = un[s, 0] - lr * un[s, 1]
            for cp in back(g, s):
                cp.start()

            @pl.when(g + 2 < NST)
            def _():
                for cp in parts(g + 2, s):
                    cp.start()

            return 0

        lax.fori_loop(0, NST, group, 0)
        for s in range(2):
            for cp in back(NST - 2 + s, s):
                cp.wait()
        copy(out, out, w_sem.at[0]).wait()


def finalize(rate, wu, gu, wd, gd, res):
    dma = pltpu.SemaphoreType.DMA
    any_ = pl.BlockSpec(memory_space=pl.ANY)
    return pl.pallas_call(
        finalize_kernel,
        out_shape=(
            jax.ShapeDtypeStruct((128, F), F32),
            jax.ShapeDtypeStruct((F, 128), F32),
            jax.ShapeDtypeStruct((TOK, D), BF),
        ),
        in_specs=[pl.BlockSpec(memory_space=pltpu.SMEM)] + [any_] * 5,
        out_specs=(any_,) * 3,
        scratch_shapes=[
            pltpu.VMEM((RING, CR, D), BF),
            pltpu.VMEM((1024, 1024), F32),
            pltpu.VMEM((CR, D), BF),
            pltpu.VMEM((2, 3, 128, QS * FC), F32),
            pltpu.VMEM((2, 3, QS * FC, 128), F32),
            dma((RING,)), dma((RING,)), dma((2, 4)), dma((2, 2)),
        ],
        compiler_params=pltpu.CompilerParams(vmem_limit_bytes=60 << 20),
        name="finalize",
    )(rate, wu, gu, wd, gd, res)


def sync_and_run(rate, wu, gu, wd, gd, rows):
    dma = pltpu.SemaphoreType.DMA
    any_ = pl.BlockSpec(memory_space=pl.ANY)
    out, _, _ = pl.pallas_call(
        kernel,
        out_shape=(
            jax.ShapeDtypeStruct((TOK, D), BF),
            jax.ShapeDtypeStruct((NCH, 2, 2, 2, 512, FC), BF),
            jax.ShapeDtypeStruct((VIA, PC, D), BF),
        ),
        in_specs=[pl.BlockSpec(memory_space=pltpu.SMEM)] + [any_] * 5,
        out_specs=(any_,) * 3,
        scratch_shapes=[
            pltpu.VMEM((R1, D), BF),
            pltpu.VMEM((R2, D), BF),
            pltpu.VMEM((R1, D), F32),
            pltpu.VMEM((2 * QS, 2, 2, 2, 512, FC), BF),
            dma((NCH,)), dma((NCH,)), dma((NCH, 4)), dma((NCH,)),
            dma(()), dma(()), dma((2,)), dma((2, 2)),
            dma((2 * QS,)), dma((2, 4)), dma((2,)), dma(()),
            dma((2,)), dma((4,)), dma((VIA,)),
        ],
        compiler_params=pltpu.CompilerParams(
            has_side_effects=True, vmem_limit_bytes=67043328, collective_id=0
        ),
        name="sync_and_run",
    )(rate, wu, gu, wd, gd, rows)
    return out


def solution(mesh):
    up_spec = P("side", None, ("rep", "tp"), None)
    down_spec = P("side", None, None, ("rep", "tp"))
    tok_spec = P("side", "rep", None, None)

    def device_step(w_up, w_down, g_up, g_down, learn_rate, prompts):
        weights = (learn_rate, w_up[0, 0], g_up[0, 0], w_down[0, 0], g_down[0, 0])
        res = sync_and_run(*weights, prompts[0, 0])
        new_up, new_down, out = finalize(*weights, res)
        return new_up[None, None], new_down[None, None], out[None, None]

    return jax.shard_map(
        device_step,
        mesh=mesh,
        in_specs=(up_spec, down_spec, up_spec, down_spec, P("side"), tok_spec),
        out_specs=(up_spec, down_spec, tok_spec),
        check_vma=False,
    )
```

```python
import functools
import math

import jax
import jax.numpy as jnp
from jax import lax
from jax.experimental import pallas as pl
from jax.experimental.pallas import tpu as pltpu
from jax.sharding import PartitionSpec as P

BF, F32 = jnp.bfloat16, jnp.float32
MESH = pl.DeviceIdType.MESH
D, F, TOK = 2048, 8192, 8192
FC = 128
NCH = F // FC
QS = 4
NST = NCH // QS
M1 = 800
R1 = QS * M1
R2 = TOK - 2 * R1
M2 = R2 // 2
PC = 40
NPC = R1 // PC
BPC = M1 // PC // 2
VIA = NPC // 2 - 1
N_A, N_B, MUL, OFF = 29, 12, 23, 17
N_G = NCH - N_A - N_B
LEAD = 13
YA, YZ, HOPS, OPP, DONE = 5, 0, (2, 4, 6), 8, 9
T_AHEAD = 3


def gelu(a):
    k = math.sqrt(2.0 / math.pi)
    half = 0.5 * a
    return half + half * jnp.tanh(a * (k + (k * 0.044715) * (a * a)))


def kernel(
    rate, wu_in, gu_in, wd_in, gd_in, rows_in, out, w_all, relay, h, h2, acc, wv,
    y_sem, x_sem, b_sem, d_sem, s_over, s_opp, s_y, s_z, ld_sem, up_sem, h_sem, o_sem,
    e_recv, e_send, r_recv,
):
    t, side, r = lax.axis_index("tp"), lax.axis_index("side"), lax.axis_index("rep")
    x, c = r // 2, r % 2

    def send(src, dst, send_sem, recv_sem, device):
        pltpu.make_async_remote_copy(
            src, dst, send_sem, recv_sem, device_id=device, device_id_type=MESH
        ).start()

    def wait(ref, sem):
        pltpu.make_async_copy(ref, ref, sem).wait()

    def kind(i, late):
        ch = jnp.clip(i - late, 0, NCH - 1)
        real = jnp.logical_and(i >= late, i < NCH + late)
        m = lax.rem((ch + OFF) * MUL, NCH)
        is_a = jnp.logical_and(real, m < N_A)
        is_g = jnp.logical_and(real, m >= N_A + N_B)
        not_a = jnp.logical_and(real, m >= N_A)
        return ch, is_a, jnp.logical_and(not_a, m < N_A + N_B), is_g, not_a

    def band(ch, col, j):
        return w_all.at[ch, c, col, :, pl.ds(j * 128, 128), :]

    def band2(ch, j):
        return w_all.at[ch, c, :, :, pl.ds(j * 128, 128), :]

    def amount(n):
        return out.at[pl.ds(0, 16 * n)]

    barrier = pltpu.get_barrier_semaphore()

    def greet(device):
        pl.semaphore_signal(barrier, inc=1, device_id=device, device_id_type=MESH)

    def greet_all(me):
        greet((t, 1 - me, r))
        greet((t, me, r ^ 2))

        @pl.when(t < 3)
        def _():
            greet((t + 1, me, r))

        @pl.when(t > 0)
        def _():
            greet((t - 1, me, r))

        for relay_t, end_t in ((1, 0), (2, 3)):

            @pl.when(t == (end_t if me else relay_t))
            def _():
                greet((relay_t if me else end_t, 1 - me, r))

    @pl.when(side == 0)
    def _():
        greet_all(0)

        def parts(g):
            s = g % 2
            f0 = pl.multiple_of(g * QS * FC, QS * FC)
            cols, rows = pl.ds(f0, QS * FC), pl.ds(f0, QS * FC)
            up, dn = pl.ds(128 * s, 128), pl.ds(512 + 512 * s, 512)
            return [
                pltpu.make_async_copy(src, dst, up_sem.at[s, k])
                for k, (src, dst) in enumerate(
                    (
                        (wu_in.at[:, cols], acc.at[up, pl.ds(0, 512)]),
                        (gu_in.at[:, cols], acc.at[up, pl.ds(512, 512)]),
                        (wd_in.at[rows, :], acc.at[dn, pl.ds(0, 128)]),
                        (gd_in.at[rows, :], acc.at[dn, pl.ds(128, 128)]),
                    )
                )
            ]

        def update(g):
            s = g % 2
            for cp in parts(g):
                cp.wait()

            @pl.when(g + 1 < NST)
            def _():
                for cp in parts(g + 1):
                    cp.start()

            lr = rate[0]
            up = pl.ds(pl.multiple_of(128 * s, 128), 128)
            new_up = (acc[up, 0:512] - lr * acc[up, 512:1024]).astype(BF)
            for q in range(QS):
                wv[QS * s + q, 0, 0, 0, 0:128, :] = new_up[:, q * FC : (q + 1) * FC]
                dn = pl.ds(pl.multiple_of(512 + 512 * s + q * FC, FC), FC)
                new_dn = (acc[dn, 0:128] - lr * acc[dn, 128:256]).astype(BF)
                wv[QS * s + q, 0, 0, 1, 0:128, :] = new_dn
            cp = pltpu.make_async_copy(
                wv.at[pl.ds(QS * s, QS), 0, 0, :, pl.ds(0, 128), :],
                w_all.at[pl.ds(QS * g, QS), c, x, :, pl.ds(t * 128, 128), :],
                o_sem,
            )
            cp.start()
            cp.wait()

        def along(ch, j, right):
            if right:
                send(band(ch, x, j), band(ch, x, j), s_z.at[0, 0], b_sem.at[ch, j], (t + 1, 0, r))
            else:
                send(band(ch, x, j), band(ch, x, j), s_z.at[1, 0], b_sem.at[ch, j], (t - 1, 0, r))

        def across(ch, col, j, k):
            send(band(ch, col, j), band(ch, col, j), s_y.at[k], y_sem.at[ch], (t, 1, r))

        def own_a(i, late):
            ch, is_a, _, _, _ = kind(i, late)

            @pl.when(is_a)
            def _():
                across(ch, x, t, 0)

                @pl.when(t < 3)
                def _():
                    along(ch, t, True)

                @pl.when(t > 0)
                def _():
                    along(ch, t, False)

        def own_z(i):
            ch, _, _, is_g, not_a = kind(i, 0)

            @pl.when(not_a)
            def _():
                across(ch, x, t, 1)

            @pl.when(is_g)
            def _():
                send(band(ch, x, t), band(ch, x, t), s_opp, x_sem.at[ch], (t, 0, r ^ 2))

        def from_opp(i):
            ch, _, _, is_g, _ = kind(i, 0)

            @pl.when(is_g)
            def _():
                wait(amount(1), x_sem.at[ch])
                across(ch, 1 - x, t, 1)

        def hop(i, late, k):
            ch, is_a, _, _, _ = kind(i, late)

            @pl.when(jnp.logical_and(is_a, t >= k))
            def _():
                wait(amount(1), b_sem.at[ch, t - k])
                across(ch, x, t - k, 0)

                @pl.when(t < 3)
                def _():
                    along(ch, t - k, True)

            @pl.when(jnp.logical_and(is_a, t + k <= 3))
            def _():
                wait(amount(1), b_sem.at[ch, t + k])
                across(ch, x, t + k, 0)

                @pl.when(t > 0)
                def _():
                    along(ch, t + k, False)

        for cp in parts(0):
            cp.start()

        def slot(i, _):
            @pl.when(jnp.logical_and(lax.rem(i, QS) == 0, i < NCH))
            def _():
                update(lax.div(i, QS))

            @pl.when(jnp.logical_and(i == 0, jnp.logical_or(t == 1, t == 2)))
            def _():
                pl.semaphore_wait(barrier, 5)

            @pl.when(jnp.logical_and(i == 0, jnp.logical_or(t == 0, t == 3)))
            def _():
                pl.semaphore_wait(barrier, 3)

            own_a(i, T_AHEAD)
            own_z(i)
            for k in (1, 2, 3):
                hop(i, T_AHEAD + k, k)
            from_opp(i)
            return 0

        lax.fori_loop(0, NCH + T_AHEAD + 3, slot, 0)

        @pl.when(jnp.logical_or(t == 1, t == 2))
        def _():
            base = jnp.where(t == 1, R1, 0)
            end = jnp.where(t == 1, 0, 3)
            odd = t - 1

            def piece(i, _):
                wait(relay.at[i], r_recv.at[i])
                half = lax.div(i, BPC) * M1 + odd * (M1 // 2)
                row = pl.multiple_of(base + half + lax.rem(i, BPC) * PC, PC)
                send(relay.at[i], out.at[pl.ds(row, PC)], e_send.at[2], e_recv.at[odd], (end, 1, r))
                return 0

            lax.fori_loop(0, VIA, piece, 0)
            wait(relay, e_send.at[2])

        wait(amount(4 * N_A), s_y.at[0])
        wait(amount(N_B + 2 * N_G), s_y.at[1])
        wait(amount(N_G), s_opp)
        for tt in range(4):

            @pl.when(t == tt)
            def _():
                if tt < 3:
                    wait(amount((tt + 1) * N_A), s_z.at[0, 0])
                if tt > 0:
                    wait(amount((4 - tt) * N_A), s_z.at[1, 0])


    @pl.when(side == 1)
    def _():
        sib, opp = (t, 1, r ^ 1), (t, 1, r ^ 2)
        greet_all(1)
        greet(sib)
        base = jnp.where(t % 2 == 0, 0, R1)

        def over(ref, ch):
            send(ref, ref, s_over, d_sem.at[ch], sib)

        def along(ch, j, right, is_b, is_g):
            k = 0 if right else 1
            dev = (t + 1, 1, r) if right else (t - 1, 1, r)

            @pl.when(is_b)
            def _():
                send(band(ch, x, j), band(ch, x, j), s_z.at[k, 0], b_sem.at[ch, j], dev)

            @pl.when(is_g)
            def _():
                send(band2(ch, j), band2(ch, j), s_z.at[k, 1], b_sem.at[ch, j], dev)

        def arrive(sem, is_b, is_g):
            @pl.when(is_b)
            def _():
                wait(amount(1), sem)

            @pl.when(is_g)
            def _():
                wait(amount(2), sem)

        def across(ch):
            own = w_all.at[ch, c, x]
            send(own, own, s_opp, x_sem.at[ch], opp)
            over(own, ch)

        def ya(i):
            ch, is_a, _, _, _ = kind(i, YA)

            @pl.when(is_a)
            def _():
                wait(amount(4), y_sem.at[ch])
                across(ch)

        def yz(i):
            ch, _, is_b, is_g, not_a = kind(i, YZ)

            @pl.when(not_a)
            def _():
                arrive(y_sem.at[ch], is_b, is_g)

                @pl.when(t < 3)
                def _():
                    along(ch, t, True, is_b, is_g)

                @pl.when(t > 0)
                def _():
                    along(ch, t, False, is_b, is_g)

        def hop(i, k):
            ch, _, is_b, is_g, not_a = kind(i, HOPS[k - 1])

            @pl.when(jnp.logical_and(not_a, t >= k))
            def _():
                arrive(b_sem.at[ch, t - k], is_b, is_g)

                @pl.when(t < 3)
                def _():
                    along(ch, t - k, True, is_b, is_g)

            @pl.when(jnp.logical_and(not_a, t + k <= 3))
            def _():
                arrive(b_sem.at[ch, t + k], is_b, is_g)

                @pl.when(t > 0)
                def _():
                    along(ch, t + k, False, is_b, is_g)

            if k == 3:

                @pl.when(is_b)
                def _():
                    across(ch)

                @pl.when(is_g)
                def _():
                    over(w_all.at[ch, c], ch)

        def from_opp(i):
            ch, is_a, is_b, _, _ = kind(i, OPP)

            @pl.when(jnp.logical_or(is_a, is_b))
            def _():
                wait(amount(4), x_sem.at[ch])
                over(w_all.at[ch, c, 1 - x], ch)

        def load(ch, ring):
            pltpu.make_async_copy(w_all.at[ch], wv.at[ring], ld_sem.at[ring]).start()

        def ready(i):
            @pl.when(jnp.logical_and(i >= DONE, i < NCH + DONE))
            def _():
                ch = jnp.clip(i - DONE, 0, NCH - 1)
                wait(amount(8), d_sem.at[ch])
                load(ch, lax.rem(ch, 2 * QS))

        def tick(i):
            ya(i)
            hop(i, 3)
            from_opp(i)
            hop(i, 2)
            yz(i)
            hop(i, 1)
            ready(i)

        def loaded(slot):
            for q in range(QS):
                wait(wv.at[QS * slot + q], ld_sem.at[QS * slot + q])

        first = pltpu.make_async_copy(
            rows_in.at[pl.ds(pl.multiple_of(base, 128), R1)], h, h_sem.at[0]
        )
        second = pltpu.make_async_copy(rows_in.at[pl.ds(2 * R1, R2)], h2, h_sem.at[1])
        first.start()
        second.start()

        def zero(i, _):
            acc[pl.ds(pl.multiple_of(i * 128, 128), 128), :] = jnp.zeros((128, D), F32)
            return 0

        lax.fori_loop(0, R1 // 128, zero, 0)
        first.wait()
        pl.semaphore_wait(barrier, 5)
        lax.fori_loop(0, LEAD, lambda i, _: (tick(i), 0)[1], 0)

        def give(i):
            for odd, (dev, there) in enumerate((((t + 1, 1, r), t < 3), ((t - 1, 1, r), t > 0))):
                row = pl.multiple_of(base + i * M1 + odd * (M1 // 2), M1 // 2)
                src = out.at[pl.ds(row, M1 // 2)]

                @pl.when(there)
                def _():
                    send(src, src, e_send.at[odd], e_recv.at[odd], dev)

                @pl.when(t == 1 + odd)
                def _():
                    def piece(q, _):
                        i2 = i * BPC + q
                        part = out.at[pl.ds(pl.multiple_of(row + q * PC, PC), PC)]

                        @pl.when(i2 < VIA)
                        def _():
                            to = jnp.minimum(i2, VIA - 1)
                            send(part, relay.at[to], e_send.at[2], r_recv.at[to], (t, 0, r))

                        @pl.when(i2 >= VIA)
                        def _():
                            end = (t + 1, 1, r) if odd else (t - 1, 1, r)
                            send(part, part, e_send.at[3], e_recv.at[odd], end)

                        return 0

                    lax.fori_loop(0, BPC, piece, 0)

        def multiply(ref, rows, slot, first=False, last=None):
            up = jnp.concatenate(
                [
                    jnp.concatenate([wv[QS * slot + q, k % 2, k // 2, 0] for q in range(QS)], axis=1)
                    for k in range(4)
                ],
                axis=0,
            )

            def down(k):
                return jnp.concatenate(
                    [
                        jnp.concatenate(
                            [
                                wv[QS * slot + q, k % 2, k // 2, 1, j * 128 : (j + 1) * 128, :]
                                for q in range(QS)
                            ],
                            axis=0,
                        )
                        for j in range(4)
                    ],
                    axis=1,
                )

            pre = jnp.dot(ref[rows[0], :], up, preferred_element_type=F32)
            for n, rs in enumerate(rows):
                if n + 1 < len(rows):
                    ahead = jnp.dot(ref[rows[n + 1], :], up, preferred_element_type=F32)
                u = gelu(pre).astype(BF)
                for k in range(4):
                    cs = pl.ds(k * 512, 512)
                    part = jnp.dot(u, down(k), preferred_element_type=F32)
                    if last is not None:
                        ref[rs, cs] = (ref[rs, cs].astype(F32) + (acc[rs, cs] + part)).astype(BF)
                        to = out.at[pl.ds(last[n], rs.size), cs]
                        pltpu.make_async_copy(ref.at[rs, cs], to, o_sem).start()
                    elif first:
                        acc[rs, cs] = part
                    else:
                        acc[rs, cs] += part
                pre = ahead if n + 1 < len(rows) else None

        def step1(sp, _):
            slot = lax.rem(sp, 2)
            loaded(slot)

            def block(i, _):
                tick(LEAD + QS * sp + i)
                multiply(h, [pl.ds(pl.multiple_of(i * M1, M1), M1)], slot)
                return 0

            lax.fori_loop(0, R1 // M1, block, 0)
            return 0

        lax.fori_loop(0, NST - 1, step1, 0)
        loaded(1)

        def last1(i, _):
            load(i, i)

            @pl.when(i > 0)
            def _():
                wait(h.at[pl.ds(0, M1)], o_sem)
                give(i - 1)

            row = pl.multiple_of(i * M1, M1)
            multiply(h, [pl.ds(row, M1)], 1, last=[pl.multiple_of(base + i * M1, M1)])
            return 0

        lax.fori_loop(0, R1 // M1, last1, 0)
        second.wait()
        loaded(0)
        for q in range(QS):
            load(QS + q, QS + q)
        halves = [pl.ds(0, M2), pl.ds(M2, M2)]
        multiply(h2, halves, 0, first=True)
        wait(h.at[pl.ds(0, M1)], o_sem)
        give(R1 // M1 - 1)

        def step2(sp, _):
            slot = lax.rem(sp, 2)
            loaded(slot)
            for q in range(QS):
                load(QS * (sp + 1) + q, QS * (1 - slot) + q)

            multiply(h2, halves, slot)
            return 0

        lax.fori_loop(1, NST - 1, step2, 0)
        loaded(1)
        multiply(h2, halves, 1, last=[2 * R1, 2 * R1 + M2])
        wait(h2, o_sem)

        half_rows = out.at[pl.ds(0, R1 // 2)]
        wait(half_rows, e_recv.at[0])
        wait(half_rows, e_recv.at[1])

        @pl.when(t < 3)
        def _():
            wait(half_rows, e_send.at[0])

        @pl.when(t > 0)
        def _():
            wait(half_rows, e_send.at[1])

        @pl.when(jnp.logical_or(t == 1, t == 2))
        def _():
            wait(out.at[pl.ds(0, VIA * PC)], e_send.at[2])
            wait(out.at[pl.ds(0, R1 // 2 - VIA * PC)], e_send.at[3])

        wait(amount(8 * NCH), s_over)
        wait(amount(4 * (N_A + N_B)), s_opp)
        for tt in range(4):

            @pl.when(t == tt)
            def _():
                if tt < 3:
                    wait(amount((tt + 1) * N_B), s_z.at[0, 0])
                    wait(amount((tt + 1) * 2 * N_G), s_z.at[0, 1])
                if tt > 0:
                    wait(amount((4 - tt) * N_B), s_z.at[1, 0])
                    wait(amount((4 - tt) * 2 * N_G), s_z.at[1, 1])


CR = 1024


def finalize_kernel(
    rate, wu_in, gu_in, wd_in, gd_in, res, up_out, dn_out, out, buf, zero, zt, ub, un, r_sem, w_sem, u_sem, v_sem
):
    side = lax.axis_index("side")

    def copy(src, dst, sem):
        return pltpu.make_async_copy(src, dst, sem)

    @pl.when(side == 1)
    def _():
        def read(i):
            return copy(res.at[pl.ds(i * CR, CR)], buf.at[i], r_sem.at[i])

        def write(i):
            return copy(buf.at[i], out.at[pl.ds(i * CR, CR)], w_sem.at[i])

        for i in range(TOK // CR):
            read(i).start()
        zero[...] = jnp.zeros_like(zero)
        for i in range(TOK // CR):
            read(i).wait()
        for i in range(TOK // CR):
            write(i).start()
        for i in range(8):
            copy(zero.at[pl.ds(0, 128)], up_out.at[:, pl.ds(i * 1024, 1024)], u_sem.at[0, 0]).start()
            copy(zero.at[:, pl.ds(0, 128)], dn_out.at[pl.ds(i * 1024, 1024)], u_sem.at[0, 1]).start()
        for i in range(TOK // CR):
            write(i).wait()
        copy(up_out, up_out, u_sem.at[0, 0]).wait()
        copy(dn_out, dn_out, u_sem.at[0, 1]).wait()

    @pl.when(side == 0)
    def _():
        w = QS * FC

        def parts(g, s):
            f = pl.ds(pl.multiple_of(g * w, w), w)
            return (
                copy(wu_in.at[:, f], ub.at[s, 0], u_sem.at[s, 0]),
                copy(gu_in.at[:, f], ub.at[s, 1], u_sem.at[s, 1]),
                copy(wd_in.at[f, :], un.at[s, 0], u_sem.at[s, 2]),
                copy(gd_in.at[f, :], un.at[s, 1], u_sem.at[s, 3]),
            )

        def back(g, s):
            f = pl.ds(pl.multiple_of(g * w, w), w)
            return (
                copy(ub.at[s, 2], up_out.at[:, f], v_sem.at[s, 0]),
                copy(un.at[s, 2], dn_out.at[f, :], v_sem.at[s, 1]),
            )

        for cp in parts(0, 0) + parts(1, 1):
            cp.start()
        zt[...] = jnp.zeros_like(zt)
        for i in range(TOK // CR):
            copy(zt, out.at[pl.ds(i * CR, CR)], w_sem.at[0]).start()
        lr = rate[0]

        def group(g, _):
            s = lax.rem(g, 2)
            for cp in parts(g, s):
                cp.wait()

            @pl.when(g >= 2)
            def _():
                for cp in back(g - 2, s):
                    cp.wait()

            ub[s, 2] = ub[s, 0] - lr * ub[s, 1]
            un[s, 2] = un[s, 0] - lr * un[s, 1]
            for cp in back(g, s):
                cp.start()

            @pl.when(g + 2 < NST)
            def _():
                for cp in parts(g + 2, s):
                    cp.start()

            return 0

        lax.fori_loop(0, NST, group, 0)
        for s in range(2):
            for cp in back(NST - 2 + s, s):
                cp.wait()
        copy(out, out, w_sem.at[0]).wait()


def finalize(rate, wu, gu, wd, gd, res):
    dma = pltpu.SemaphoreType.DMA
    any_ = pl.BlockSpec(memory_space=pl.ANY)
    return pl.pallas_call(
        finalize_kernel,
        out_shape=(
            jax.ShapeDtypeStruct((128, F), F32),
            jax.ShapeDtypeStruct((F, 128), F32),
            jax.ShapeDtypeStruct((TOK, D), BF),
        ),
        in_specs=[pl.BlockSpec(memory_space=pltpu.SMEM)] + [any_] * 5,
        out_specs=(any_,) * 3,
        scratch_shapes=[
            pltpu.VMEM((TOK // CR, CR, D), BF),
            pltpu.VMEM((1024, 1024), F32),
            pltpu.VMEM((CR, D), BF),
            pltpu.VMEM((2, 3, 128, QS * FC), F32),
            pltpu.VMEM((2, 3, QS * FC, 128), F32),
            dma((TOK // CR,)), dma((TOK // CR,)), dma((2, 4)), dma((2, 2)),
        ],
        compiler_params=pltpu.CompilerParams(vmem_limit_bytes=60 << 20),
        name="finalize",
    )(rate, wu, gu, wd, gd, res)


def sync_and_run(rate, wu, gu, wd, gd, rows):
    dma = pltpu.SemaphoreType.DMA
    any_ = pl.BlockSpec(memory_space=pl.ANY)
    out, _, _ = pl.pallas_call(
        kernel,
        out_shape=(
            jax.ShapeDtypeStruct((TOK, D), BF),
            jax.ShapeDtypeStruct((NCH, 2, 2, 2, 512, FC), BF),
            jax.ShapeDtypeStruct((VIA, PC, D), BF),
        ),
        in_specs=[pl.BlockSpec(memory_space=pltpu.SMEM)] + [any_] * 5,
        out_specs=(any_,) * 3,
        scratch_shapes=[
            pltpu.VMEM((R1, D), BF),
            pltpu.VMEM((R2, D), BF),
            pltpu.VMEM((R1, D), F32),
            pltpu.VMEM((2 * QS, 2, 2, 2, 512, FC), BF),
            dma((NCH,)), dma((NCH,)), dma((NCH, 4)), dma((NCH,)),
            dma(()), dma(()), dma((2,)), dma((2, 2)),
            dma((2 * QS,)), dma((2, 4)), dma((2,)), dma(()),
            dma((2,)), dma((4,)), dma((VIA,)),
        ],
        compiler_params=pltpu.CompilerParams(
            has_side_effects=True, vmem_limit_bytes=67043328, collective_id=0
        ),
        name="sync_and_run",
    )(rate, wu, gu, wd, gd, rows)
    return out


def solution(mesh):
    up_spec = P("side", None, ("rep", "tp"), None)
    down_spec = P("side", None, None, ("rep", "tp"))
    tok_spec = P("side", "rep", None, None)

    def device_step(w_up, w_down, g_up, g_down, learn_rate, prompts):
        weights = (learn_rate, w_up[0, 0], g_up[0, 0], w_down[0, 0], g_down[0, 0])
        res = sync_and_run(*weights, prompts[0, 0])
        new_up, new_down, out = finalize(*weights, res)
        return new_up[None, None], new_down[None, None], out[None, None]

    return jax.shard_map(
        device_step,
        mesh=mesh,
        in_specs=(up_spec, down_spec, up_spec, down_spec, P("side"), tok_spec),
        out_specs=(up_spec, down_spec, tok_spec),
        check_vma=False,
    )
```
